128 devices in a mesh: grp: 2 (over core), row: 8 (over z, y_hi), col: 8 (over y_lo, x).
Axes of the slice: x: 4, y: 4 (y_hi: 2, y_lo: 2; y = y_hi * 2 + y_lo), z: 4, core: 2. Of those that a mesh axis runs over, the one named last changes fastest.
Arguments:
- ainv_anc: bfloat16 [12288, 12288], P(('grp', 'row'), 'col'), may hold values from -12 to 12
- l_upper: bfloat16 [12288, 2048], P(('grp', 'row'), 'col'), may hold values from -0.0546875 to 0.0546875
- mask_upper: int32 [8, 48], replicated, may hold values from 0 to 1, as said below
- dinv_upper: float32 [256, 2048], P(None, 'col'), may hold values from -6 to 6
- l_lower: bfloat16 [12288, 2048], P(('grp', 'row'), 'col'), may hold values from -0.0546875 to 0.0546875
- mask_lower: int32 [8, 48], replicated, may hold values from 0 to 1, as said below
- parent: int32 [8], replicated, may hold values from 0 to 7
- lp_lower: bfloat16 [256, 2048], P(None, 'col'), may hold values from -0.375 to 0.375
- dinv_lower: float32 [256, 2048], P(None, 'col'), may hold values from -6 to 6
Outputs:
- x_upper: bfloat16 [12288, 2048], P(('grp', 'row'), 'col')
- diag_upper: bfloat16 [256, 2048], P(None, 'col')
- y_lower: bfloat16 [12288, 2048], P(('grp', 'row'), 'col')
- y_parent: bfloat16 [256, 2048], P(None, 'col')
- diag_lower: bfloat16 [256, 2048], P(None, 'col')
The draws below stay inside these ranges and needn't reach their ends.
Inputs may be any that keep to these rules, and one draw needn't show every extreme that they name: mask_upper[u, a] is 1 where ancestor block a lies in the structure of upper supernode u. mask_lower[l, a] is 1 where ancestor block a lies in the structure of lower supernode l. parent[l] is the upper supernode whose columns hold lower supernode l's parent block.
All inputs are finite; a program needn't handle non-finite values.
Results may differ from the reference program's by a relative error of at most 0.0095.
Values may be sent and summed in bfloat16 or wider, within the bound.
A program may use at most 128 MiB of HBM per device.

```python
import jax
import jax.numpy as jnp
from jax import lax

B = 256
ANC = 12288
ANCB = 48
SN = 8


def draw_ainv_anc(key, part):
    entry_key, diag_key = jax.random.split(key, 2)
    entries = jnp.clip(jax.random.normal(entry_key, (ANC, ANC), jnp.float32), -7.0, 7.0)
    diagonal = jnp.exp(jax.random.uniform(diag_key, (ANC,), jnp.float32, 0.0, 1.386))
    places = jnp.arange(ANC)
    return entries.at[places, places].add(diagonal).astype(jnp.bfloat16)


def pattern_draw(key):
    chance = jax.random.randint(key, (SN, ANCB), 0, 1000)
    threshold = 250 + 650 * jnp.arange(ANCB, dtype=jnp.int32) // max(ANCB - 1, 1)
    return (chance < threshold[None, :]).astype(jnp.int32)


def draw_mask_upper(key, part):
    return pattern_draw(jax.random.fold_in(key, 17))


def draw_mask_lower(key, part):
    return pattern_draw(jax.random.fold_in(key, 29))


def plant(drawn, own_key, smallest, high):
    dims = drawn.shape
    place = [jax.random.randint(jax.random.fold_in(own_key, axis), (), 0, dims[axis]) for axis in range(len(dims))]
    drawn = drawn.at[tuple(place)].set(smallest)
    longest = dims.index(max(dims))
    place[longest] = (place[longest] + 1) % dims[longest]
    return drawn.at[tuple(place)].set(high)


def levels(stream_key, shape, cuts, smallest, high):
    def one(position, shards_of):
        heights = jax.random.uniform(jax.random.fold_in(jax.random.fold_in(stream_key, 6), position), (shards_of,), jnp.float32, smallest / len(cuts), high / len(cuts))
        return jnp.repeat(jnp.exp(heights), shape[position] // shards_of).reshape((-1,) + (1,) * (len(shape) - position - 1))

    gain = one(*cuts[0])
    for cut in cuts[1:]:
        gain = gain * one(*cut)
    return gain


def noise(rng, extent, width, bound, cuts=(), kind=jnp.bfloat16):
    values = jax.random.normal(rng, extent, jnp.float32) * width
    if len(cuts) > 0:
        values = levels(rng, extent, cuts, -0.22, 0.18) * values
    return jnp.clip(values, min=-bound, max=bound).astype(kind)


def setup_inputs(seed: int = 0) -> dict:
    keys = jax.random.split(jax.random.key(seed), 10)
    return {
        "ainv_anc": draw_ainv_anc(jax.random.fold_in(keys[9], 71), 0),
        "l_upper": noise(keys[1], (ANC, SN * B), ANC ** -0.5, 0.0546875, ((0, 16), (1, 8))),
        "mask_upper": draw_mask_upper(jax.random.fold_in(keys[9], 71), 0),
        "dinv_upper": noise(keys[3], (B, SN * B), 1.0, 6.0, ((1, 8),), jnp.float32),
        "l_lower": noise(keys[4], (ANC, SN * B), ANC ** -0.5, 0.0546875, ((0, 16), (1, 8))),
        "mask_lower": draw_mask_lower(jax.random.fold_in(keys[9], 71), 0),
        "parent": plant(jax.random.randint(keys[6], (SN,), 0, SN), jax.random.fold_in(keys[6], 1), 0, SN - 1).astype(jnp.int32),
        "lp_lower": noise(keys[7], (B, SN * B), B ** -0.5, 0.375, ((1, 8),)),
        "dinv_lower": noise(keys[8], (B, SN * B), 1.0, 6.0, ((1, 8),), jnp.float32),
    }


def masked_panel(factor, pattern):
    height, breadth = factor.shape
    shaped = factor.reshape(height // B, B, breadth // B, B)
    keeping = (jnp.transpose(pattern) > 0)[:, None, :, None]
    return jnp.where(keeping, shaped, jnp.zeros((), factor.dtype)).reshape(height, breadth)


def reference(ainv_anc, l_upper, mask_upper, dinv_upper, l_lower, mask_lower, parent, lp_lower, dinv_lower):
    precise = lax.Precision.HIGHEST
    ancestor = ainv_anc.astype(jnp.float32)
    upper_masked = masked_panel(l_upper, mask_upper)
    x_upper = (-jnp.dot(ancestor, upper_masked.astype(jnp.float32), precision=precise)).astype(jnp.bfloat16)
    upper_cube = upper_masked.astype(jnp.float32).reshape(ANC, SN, B)
    x_cube = x_upper.astype(jnp.float32).reshape(ANC, SN, B)
    upper_terms = jnp.einsum("aub,auc->buc", upper_cube, x_cube, precision=precise).reshape(B, SN * B)
    diag_upper = (dinv_upper - upper_terms).astype(jnp.bfloat16)
    lower_masked = masked_panel(l_lower, mask_lower)
    lower_cube = lower_masked.astype(jnp.float32).reshape(ANC, SN, B)
    chosen = jnp.take(x_cube, parent, axis=1)
    link_cube = lp_lower.astype(jnp.float32).reshape(B, SN, B)
    coupling = jnp.einsum("alb,blc->alc", chosen, link_cube, precision=precise).reshape(ANC, SN * B)
    lower_sum = jnp.dot(ancestor, lower_masked.astype(jnp.float32), precision=precise)
    y_lower = (-(lower_sum + coupling)).astype(jnp.bfloat16)
    y_cube = y_lower.astype(jnp.float32).reshape(ANC, SN, B)
    crossed = jnp.einsum("alb,alc->blc", chosen, lower_cube, precision=precise)
    own_terms = jnp.einsum("alb,alc->blc", lower_cube, y_cube, precision=precise)
    parent_diag = jnp.take(diag_upper.astype(jnp.float32).reshape(B, SN, B), parent, axis=1)
    parent_terms = jnp.einsum("blc,cld->bld", parent_diag, link_cube, precision=precise)
    y_parent = (-(crossed + parent_terms)).astype(jnp.bfloat16)
    parent_cube = y_parent.astype(jnp.float32)
    back_terms = jnp.einsum("clb,cld->bld", link_cube, parent_cube, precision=precise)
    diag_lower = (dinv_lower.reshape(B, SN, B) - own_terms - back_terms).astype(jnp.bfloat16)
    return x_upper, diag_upper, y_lower, y_parent.reshape(B, SN * B), diag_lower.reshape(B, SN * B)
```

```python
import functools

import jax
import jax.numpy as jnp
from jax import lax
from jax.experimental import pallas as pl
from jax.experimental.pallas import tpu as pltpu
from jax.sharding import PartitionSpec as P

B = 256
H = 128
MESH = pl.DeviceIdType.MESH
F32 = jnp.float32
BF16 = jnp.bfloat16


def place():
    g, row, col = lax.axis_index("grp"), lax.axis_index("row"), lax.axis_index("col")
    return g, row, col, row // 2, row % 2, col // 4, col % 4


def device(g, x, h, b, z):
    return (g, z * 2 + h, b * 4 + x)


def remote(src, dst, send, recv, target):
    return pltpu.make_async_remote_copy(
        src_ref=src, dst_ref=dst, send_sem=send, recv_sem=recv, device_id=target, device_id_type=MESH
    )


def main_kernel(
    lh, a_hbm, out, a_own, a_oth, s1, panel, part, r1, r2, kept, yb,
    a_sem, as_sem, ar_sem, s1s, s1r, s2s, s2r, ags, agr, p1s, p1r, p2s, p2r, p3s, p3r,
):
    g, row, col, z, h, b, x = place()
    rows = a_own.shape[0]
    quarter, sl, half = rows // 4, rows // 8, rows // 2
    chunks = panel.shape[0]

    local_a = pltpu.make_async_copy(a_hbm, a_own, a_sem)
    local_a.start()
    other = (1 - g, row, col)
    swap_a = remote(a_hbm, a_oth, as_sem, ar_sem, other)

    def first(pn, dz, dg):
        gt, zt = (g + dg) % 2, (z + dz) % 4
        return remote(
            lh.at[gt, pn, zt], s1.at[g, z, pn], s1s.at[pn, dg * 4 + dz], s1r.at[pn, g * 4 + z],
            device(gt, x, h, b, zt),
        )

    def first_in(pn, dz, dg):
        gs, zs = (g + dg) % 2, (z + dz) % 4
        return gs, zs, remote(
            lh.at[g, pn, z], s1.at[gs, zs, pn], s1s.at[pn, 0], s1r.at[pn, gs * 4 + zs], device(g, x, h, b, z)
        )

    order = [(dz, dg) for dz in (2, 1, 3, 0) for dg in (0, 1)]
    for pn in range(2):
        for dz, dg in order:
            if (dz, dg) != (0, 0):
                first(pn, dz, dg).start()
        s1[g, z, pn] = lh[g, pn, z]
        if pn == 0:
            swap_a.start()

    def second(pn, dx, dg, dh):
        zs, gs, ht = (x + dx) % 4, (b + dg) % 2, (h + dh) % 2
        spot = panel.at[
            pn * 4 + col // 2,
            pl.ds(pl.multiple_of(h * rows + z * quarter, 16), quarter),
            pl.ds(pl.multiple_of((col % 2) * H, H), H),
        ]
        return zs, gs, remote(
            s1.at[gs, zs, pn], spot, s2s.at[pn, dx * 4 + dg * 2 + dh], s2r.at[pn, h * 8 + col],
            device(g, zs, ht, gs, z),
        )

    for pn in range(2):
        for dz, dg in order:
            if (dz, dg) != (0, 0):
                first_in(pn, dz, dg)[2].wait_recv()
        for dx in (2, 1, 3, 0):
            for dg in range(2):
                for dh in range(2):
                    zs, gs, copy = second(pn, dx, dg, dh)
                    if (dx, dg, dh) != (0, 0, 0):
                        copy.start()
                    else:
                        panel[
                            pn * 4 + col // 2,
                            pl.ds(pl.multiple_of(h * rows + z * quarter, 16), quarter),
                            pl.ds(pl.multiple_of((col % 2) * H, H), H),
                        ] = s1[gs, zs, pn]

    def second_in(m, e, hs):
        cs = (m % 4) * 2 + e
        spot = panel.at[
            m, pl.ds(pl.multiple_of(hs * rows + z * quarter, 16), quarter), pl.ds(e * H, H)
        ]
        pn = m // 4
        return cs, remote(
            s1.at[0, 0, 0], spot, s2s.at[pn, 0], s2r.at[pn, hs * 8 + cs], device(g, x, h, b, z)
        )

    right = device(g, x, h, b, (z + 1) % 4)
    left = device(g, x, h, b, (z + 3) % 4)

    def spot_of(m, hs, q):
        return panel.at[m, pl.ds(pl.multiple_of(hs * rows + q * quarter, 16), quarter)]

    def gather(m, slot, q, hs, to):
        return remote(spot_of(m, hs, q), spot_of(m, hs, q), ags.at[m, slot], agr.at[m, slot], to)

    def step_a(m):
        for hs in range(2):
            for e in range(2):
                cs, copy = second_in(m, e, hs)

                @pl.when(jnp.logical_not((cs == col) & (hs == h)))
                def _():
                    copy.wait_recv()

        for hs in range(2):
            gather(m, hs, z, hs, right).start()
            gather(m, 2 + hs, z, hs, left).start()

    def step_b(m):
        gather(m, 0, (z + 3) % 4, 0, right).wait_recv()
        gather(m, 4, (z + 3) % 4, 0, right).start()
        gather(m, 3, (z + 1) % 4, 1, left).wait_recv()
        gather(m, 5, (z + 1) % 4, 1, left).start()

    xr = device(g, (x + 1) % 4, h, b, z)
    xl = device(g, (x + 3) % 4, h, b, z)
    far = (x + 2) % 4

    def half_copy(m, way):
        return remote(
            part.at[m, far, way], r1.at[m, way], p1s.at[m, way], p1r.at[m, way], xr if way == 0 else xl
        )

    def full_copy(m, way):
        near = (x + 1) % 4 if way == 0 else (x + 3) % 4
        return remote(
            part.at[m, near], r2.at[m, way], p2s.at[m, way], p2r.at[m, way], xr if way == 0 else xl
        )

    def pair_copy(m):
        return remote(
            r2.at[m, 0, :, 1 - b], yb.at[m], p3s.at[m], p3r.at[m], device(g, x, h, 1 - b, z)
        )

    def step_c(m):
        gather(m, 1, (z + 3) % 4, 1, right).wait_recv()
        gather(m, 2, (z + 1) % 4, 0, left).wait_recv()
        gather(m, 4, far_z, 0, right).wait_recv()
        gather(m, 5, far_z, 1, left).wait_recv()
        for o, a in enumerate((a_own, a_oth)):
            for bt in range(2):
                product = jnp.dot(
                    a[bt * half:(bt + 1) * half, :], panel[m], preferred_element_type=F32
                ).astype(BF16)
                for xt in range(4):
                    part[m, xt, o, bt] = product[xt * sl:(xt + 1) * sl]
        half_copy(m, 0).start()
        half_copy(m, 1).start()

    def step_d(m):
        for way in range(2):
            near = (x + 1) % 4 if way == 0 else (x + 3) % 4
            half_copy(m, way).wait_recv()
            part[m, near, way] = (part[m, near, way].astype(F32) + r1[m, way].astype(F32)).astype(BF16)
            full_copy(m, way).start()

    def step_e(m):
        full_copy(m, 0).wait_recv()
        full_copy(m, 1).wait_recv()
        for bt in range(2):
            total = (
                part[m, x, :, bt].astype(F32) + r2[m, 0, :, bt].astype(F32) + r2[m, 1, :, bt].astype(F32)
            )
            r2[m, 0, :, bt] = total.astype(BF16)

            @pl.when(b == bt)
            def _():
                kept[m] = total

        pair_copy(m).start()

    def step_f(m):
        pair_copy(m).wait_recv()
        total = -(kept[m] + yb[m].astype(F32))
        result = total.astype(BF16)
        out[2 * m] = result[:, :, :H]
        out[2 * m + 1] = result[:, :, H:]

    far_z = (z + 2) % 4
    local_a.wait()
    swap_a.wait_recv()

    steps = (step_a, step_b, step_c, step_d, step_e, step_f)

    def body(t, carry):
        for k, step in enumerate(steps):
            m = t - k

            @pl.when((m >= 0) & (m < chunks))
            def _(step=step, m=m):
                step(m)

        return carry

    lax.fori_loop(0, chunks + len(steps) - 1, body, 0)

    swap_a.wait_send()
    for pn in range(2):
        for dz, dg in order:
            if (dz, dg) != (0, 0):
                first(pn, dz, dg).wait_send()
        for dx in range(4):
            for dg in range(2):
                for dh in range(2):
                    if (dx, dg, dh) != (0, 0, 0):
                        second(pn, dx, dg, dh)[2].wait_send()

    def drain(m, carry):
        for hs in range(2):
            gather(m, hs, z, hs, right).wait_send()
            gather(m, 2 + hs, z, hs, left).wait_send()
        gather(m, 4, z, 0, right).wait_send()
        gather(m, 5, z, 1, left).wait_send()
        for way in range(2):
            half_copy(m, way).wait_send()
            full_copy(m, way).wait_send()
        pair_copy(m).wait_send()
        return carry

    lax.fori_loop(0, chunks, drain, 0)


def main_call(lh, a):
    rows, depth = a.shape
    quarter, sl = rows // 4, rows // 8
    chunks = 8
    dma = pltpu.SemaphoreType.DMA
    return pl.pallas_call(
        main_kernel,
        out_shape=jax.ShapeDtypeStruct((16, 2, sl, H), BF16),
        in_specs=[pl.BlockSpec(memory_space=pltpu.VMEM), pl.BlockSpec(memory_space=pl.ANY)],
        out_specs=pl.BlockSpec(memory_space=pltpu.VMEM),
        scratch_shapes=[
            pltpu.VMEM((rows, depth), BF16),
            pltpu.VMEM((rows, depth), BF16),
            pltpu.VMEM((2, 4, 2, quarter, H), BF16),
            pltpu.VMEM((chunks, depth, B), BF16),
            pltpu.VMEM((chunks, 4, 2, 2, sl, B), BF16),
            pltpu.VMEM((chunks, 2, 2, sl, B), BF16),
            pltpu.VMEM((chunks, 2, 2, 2, sl, B), BF16),
            pltpu.VMEM((chunks, 2, sl, B), F32),
            pltpu.VMEM((chunks, 2, sl, B), BF16),
            dma, dma, dma,
            dma((2, 8)), dma((2, 8)),
            dma((2, 16)), dma((2, 16)),
            dma((chunks, 6)), dma((chunks, 6)),
            dma((chunks, 2)), dma((chunks, 2)),
            dma((chunks, 2)), dma((chunks, 2)),
            dma((chunks,)), dma((chunks,)),
        ],
        compiler_params=pltpu.CompilerParams(has_side_effects=True, vmem_limit_bytes=60 * 2**20),
        name="panels",
    )(lh, a)


def tail_kernel(
    parent, slices, mu, ml, lp, du_in, dl_in,
    x_out, y_out, du_out, yp_out, dl_out,
    chosen_s, xt, ct, st, red_s, red, dcol, back,
    ts, tr, rs, rr, cs, cr, gs, gr,
):
    g, row, col, z, h, b, x = place()
    me = g * 8 + row
    sl = slices.shape[2]
    n_r, n_c = 16, 8
    deep = B // n_r

    for c in range(n_c):
        chosen_s[c] = slices[parent[c]]

    mine = pl.ds(pl.multiple_of(col * sl, 16), sl)
    lanes = pl.ds(pl.multiple_of(g * H, H), H)
    kinds = (xt, ct, st)

    def source(k, c, o):
        if k == 0:
            return slices.at[c, o]
        if k == 1:
            return chosen_s.at[c, o]
        return slices.at[8 + c, o]

    def turn(k, i):
        dc, o = i // 2, i % 2
        c = (col + dc) % n_c
        return remote(
            source(k, c, o), kinds[k].at[mine, lanes], ts.at[k, i], tr.at[k, g * 8 + col],
            ((g + o) % 2, row, c),
        )

    def turn_in(k, i):
        dc, o = i // 2, i % 2
        c, gg = (col + dc) % n_c, (g + o) % 2
        return remote(
            source(k, 0, 0),
            kinds[k].at[pl.ds(pl.multiple_of(c * sl, 16), sl), pl.ds(pl.multiple_of(gg * H, H), H)],
            ts.at[k, 0], tr.at[k, gg * 8 + c], (g, row, col),
        )

    def loop(lo, hi, f):
        def body(i, carry):
            f(i)
            return carry

        lax.fori_loop(lo, hi, body, 0)

    for k in range(3):
        loop(1, 16, lambda i, k=k: turn(k, i).start())
    xt[mine, lanes] = slices[col, 0]
    ct[mine, lanes] = chosen_s[col, 0]
    st[mine, lanes] = slices[8 + col, 0]

    def peer(d):
        r = (me + d) % n_r
        return r, (r // 8, r % 8, col)

    def scatter(k, d):
        r, to = peer(d)
        return remote(red_s.at[k, r], red.at[k, me], rs.at[k, d], rr.at[k, me], to)

    def scatter_in(k, d):
        r, _ = peer(d)
        return remote(red_s.at[k, r], red.at[k, r], rs.at[k, d], rr.at[k, r], (g, row, col))

    def reduce_start(k, value):
        red_s[k] = value.reshape(n_r, deep, B).astype(BF16)
        loop(1, n_r, lambda d: scatter(k, d).start())
        red[k, me] = red_s[k, me]

    def reduce_end(k):
        loop(1, n_r, lambda d: scatter_in(k, d).wait_recv())
        return jnp.sum(red[k].astype(F32), axis=0)

    outs = (du_out, yp_out, dl_out)

    def spread(k, d):
        r, to = peer(d)
        return remote(outs[k].at[me], outs[k].at[me], gs.at[k, d], gr.at[k, me], to)

    def spread_in(k, d):
        r, _ = peer(d)
        return remote(outs[k].at[r], outs[k].at[r], gs.at[k, d], gr.at[k, r], (g, row, col))

    def flipped(p, q):
        return lax.dot_general(p, q, (((0,), (0,)), ((), ())), preferred_element_type=F32)

    loop(1, 16, lambda i: turn_in(0, i).wait_recv())
    x_out[...] = xt[...]
    reduce_start(0, flipped(mu[...], xt[...]))
    loop(1, 16, lambda i: turn_in(1, i).wait_recv())
    reduce_start(1, flipped(ct[...], ml[...]))
    loop(1, 16, lambda i: turn_in(2, i).wait_recv())
    y = (st[...].astype(F32) - jnp.dot(ct[...], lp[...], preferred_element_type=F32)).astype(BF16)
    y_out[...] = y
    reduce_start(2, flipped(ml[...], y))

    du = (du_in[me] - reduce_end(0)).astype(BF16)
    du_out[me] = du
    dcol[col] = du
    loop(1, n_r, lambda d: spread(0, d).start())

    def column(d):
        c = (col + d) % n_c
        return remote(dcol.at[col], dcol.at[col], cs.at[d], cr.at[col], (g, row, c))

    def column_in(d):
        c = (col + d) % n_c
        return remote(dcol.at[c], dcol.at[c], cs.at[d], cr.at[c], (g, row, col))

    loop(1, n_c, lambda d: column(d).start())
    crossed = reduce_end(1)
    loop(1, n_c, lambda d: column_in(d).wait_recv())
    own = dcol[parent[col]]
    yp_out[me] = (-(crossed + jnp.dot(own, lp[...], preferred_element_type=F32))).astype(BF16)
    loop(1, n_r, lambda d: spread(1, d).start())
    lower = dl_in[me] - reduce_end(2)
    loop(1, n_r, lambda d: spread_in(1, d).wait_recv())
    back[...] = flipped(lp[...], yp_out[...].reshape(B, B)).reshape(n_r, deep, B)
    dl_out[me] = (lower - back[me]).astype(BF16)
    loop(1, n_r, lambda d: spread(2, d).start())
    loop(1, n_r, lambda d: spread_in(0, d).wait_recv())
    loop(1, n_r, lambda d: spread_in(2, d).wait_recv())

    for k in range(3):
        loop(1, 16, lambda i, k=k: turn(k, i).wait_send())
        loop(1, n_r, lambda d, k=k: scatter(k, d).wait_send())
        loop(1, n_r, lambda d, k=k: spread(k, d).wait_send())
    loop(1, n_c, lambda d: column(d).wait_send())


def tail_call(parent, slices, mu, ml, lp, du, dl):
    rows = mu.shape[0]
    dma = pltpu.SemaphoreType.DMA
    vmem = pl.BlockSpec(memory_space=pltpu.VMEM)
    deep = B // 16
    block = jax.ShapeDtypeStruct((rows, B), BF16)
    square = jax.ShapeDtypeStruct((16, deep, B), BF16)
    x, y, d_u, y_p, d_l = pl.pallas_call(
        tail_kernel,
        out_shape=(block, block, square, square, square),
        in_specs=[pl.BlockSpec(memory_space=pltpu.SMEM)] + [vmem] * 6,
        out_specs=(vmem,) * 5,
        scratch_shapes=[
            pltpu.VMEM((8,) + slices.shape[1:], BF16),
            pltpu.VMEM((rows, B), BF16),
            pltpu.VMEM((rows, B), BF16),
            pltpu.VMEM((rows, B), BF16),
            pltpu.VMEM((3, 16, deep, B), BF16),
            pltpu.VMEM((3, 16, deep, B), BF16),
            pltpu.VMEM((8, deep, B), BF16),
            pltpu.VMEM((16, deep, B), F32),
            dma((3, 16)), dma((3, 16)),
            dma((3, 16)), dma((3, 16)),
            dma((8,)), dma((8,)),
            dma((3, 16)), dma((3, 16)),
        ],
        compiler_params=pltpu.CompilerParams(has_side_effects=True, vmem_limit_bytes=40 * 2**20),
        name="tail",
    )(parent, slices, mu, ml, lp, du.reshape(16, deep, B), dl.reshape(16, deep, B))
    return x, d_u.reshape(B, B), y, y_p.reshape(B, B), d_l.reshape(B, B)


def step(a, lu, mask_u, du, ll, mask_l, parent, lp, dl):
    g, row, col = lax.axis_index("grp"), lax.axis_index("row"), lax.axis_index("col")
    rows = a.shape[0]
    blocks = max(rows // B, 1)
    base = (g * 8 + row) * rows

    def masked(factor, mask):
        line = lax.dynamic_slice(mask, (col, 0), (1, mask.shape[1]))[0]
        keep = line[(base + jnp.arange(rows)) // B]
        return jnp.where(keep[:, None] > 0, factor, jnp.zeros((), factor.dtype))

    mu, ml = masked(lu, mask_u), masked(ll, mask_l)
    both = jnp.stack([mu, ml]).reshape(2, 4, rows // 4, 2, H)
    lh = jnp.transpose(both, (3, 0, 1, 2, 4))
    slices = main_call(lh, a)
    return tail_call(parent, slices, mu, ml, lp, du, dl)


def solution(mesh):
    rows, cols = P(("grp", "row"), "col"), P(None, "col")
    none = P(None, None)
    return jax.shard_map(
        step,
        mesh=mesh,
        in_specs=(rows, rows, none, cols, rows, none, P(None), cols, cols),
        out_specs=(rows, cols, rows, cols, cols),
        check_vma=False,
    )
```

```python
import jax
import jax.numpy as jnp
from jax import lax
from jax.experimental import pallas as pl
from jax.experimental.pallas import tpu as pltpu
from jax.sharding import PartitionSpec as P

B = 256
H = 128
CH = 8
NS = 16
MESH = pl.DeviceIdType.MESH
F32 = jnp.float32
BF16 = jnp.bfloat16


def device(g, x, h, b, z):
    return (g, z * 2 + h, b * 4 + x)


def remote(src, dst, send, recv, target):
    return pltpu.make_async_remote_copy(
        src_ref=src, dst_ref=dst, send_sem=send, recv_sem=recv, device_id=target, device_id_type=MESH
    )


def aligned(start, size):
    return pl.ds(pl.multiple_of(start, size), size)


def loop(lo, hi, f):
    def body(i, carry):
        f(i)
        return carry

    lax.fori_loop(lo, hi, body, 0)


def flipped(p, q):
    return lax.dot_general(p, q, (((0,), (0,)), ((), ())), preferred_element_type=F32)


def kernel(
    mask_u, mask_l, parent, lu, ll, a_hbm, lp, du_in, dl_in,
    x_out, y_out, du_out, yp_out, dl_out,
    masked, a, s1, panel, part, r1, r2, kept, yb, xs, chosen_s, xst, ct, cl, red_s, red, dcol, back,
    a_sem, as_sem, ar_sem, s1s, s1r, s2s, s2r, ags, agr, p1s, p1r, p2s, p2r, p3s, p3r,
    ts, tr, rs, rr, cs, cr, gs, gr,
):
    g, row, col = lax.axis_index("grp"), lax.axis_index("row"), lax.axis_index("col")
    z, h, b, x = row // 2, row % 2, col // 4, col % 4
    me = g * 8 + row
    rows = a.shape[1]
    quarter, sl, half = rows // 4, rows // 8, rows // 2
    bl = min(B, rows)
    here = (g, row, col)

    for pn, (factor, mask) in enumerate(((lu, mask_u), (ll, mask_l))):
        for i in range(rows // bl):
            keep = mask[col, (me * rows + i * bl) // B] > 0
            values = factor[i * bl:(i + 1) * bl, :]
            masked[pn, i * bl:(i + 1) * bl, :] = jnp.where(keep, values, jnp.zeros_like(values))

    local_a = pltpu.make_async_copy(a_hbm, a.at[0], a_sem)
    local_a.start()
    swap_a = remote(a_hbm, a.at[1], as_sem, ar_sem, (1 - g, row, col))

    def piece(pn, q, half_of):
        return masked.at[pn, aligned(q * quarter, quarter), aligned(half_of * H, H)]

    def first(pn, dz, dg):
        gt, zt = (g + dg) % 2, (z + dz) % 4
        return remote(
            piece(pn, zt, gt), s1.at[g, z, pn], s1s.at[pn, dg * 4 + dz], s1r.at[pn, g * 4 + z],
            device(gt, x, h, b, zt),
        )

    def first_in(pn, dz, dg):
        gf, zf = (g + dg) % 2, (z + dz) % 4
        return remote(piece(pn, z, g), s1.at[gf, zf, pn], s1s.at[pn, 0], s1r.at[pn, gf * 4 + zf], here)

    order = [(dz, dg) for dz in (2, 1, 3, 0) for dg in (0, 1)]
    for pn in range(2):
        for dz, dg in order:
            if (dz, dg) != (0, 0):
                first(pn, dz, dg).start()
        s1[g, z, pn] = masked[pn, aligned(z * quarter, quarter), aligned(g * H, H)]
        if pn == 0:
            swap_a.start()

    def spot_from(pn, hf, cf, lane):
        return (pn * 4 + cf // 2, aligned(hf * rows + z * quarter, quarter), lane)

    def second(pn, dx, dg, dh):
        zf, gf, ht = (x + dx) % 4, (b + dg) % 2, (h + dh) % 2
        return zf, gf, remote(
            s1.at[gf, zf, pn], panel.at[spot_from(pn, h, col, aligned((col % 2) * H, H))],
            s2s.at[pn, dx * 4 + dg * 2 + dh], s2r.at[pn, h * 8 + col], device(g, zf, ht, gf, z),
        )

    far_first = [(dx, dg, dh) for dx in (2, 1, 3, 0) for dg in range(2) for dh in range(2)]
    for pn in range(2):
        for dz, dg in order:
            if (dz, dg) != (0, 0):
                first_in(pn, dz, dg).wait_recv()
        for way in far_first:
            zf, gf, copy = second(pn, *way)
            if way != (0, 0, 0):
                copy.start()
            else:
                panel[spot_from(pn, h, col, aligned((col % 2) * H, H))] = s1[gf, zf, pn]

    right, left = device(g, x, h, b, (z + 1) % 4), device(g, x, h, b, (z + 3) % 4)
    far_z = (z + 2) % 4

    def gather(m, slot, q, hf, to):
        spot = panel.at[m, aligned(hf * rows + q * quarter, quarter)]
        return remote(spot, spot, ags.at[m, slot], agr.at[m, slot], to)

    def step_a(m):
        pn = m // 4
        for hf in range(2):
            for e in range(2):
                cf = (m % 4) * 2 + e
                copy = remote(
                    s1.at[0, 0, 0], panel.at[spot_from(pn, hf, cf, pl.ds(e * H, H))],
                    s2s.at[pn, 0], s2r.at[pn, hf * 8 + cf], here,
                )
                pl.when(jnp.logical_not((cf == col) & (hf == h)))(copy.wait_recv)
        for hf in range(2):
            gather(m, hf, z, hf, right).start()
            gather(m, 2 + (1 - hf), z, 1 - hf, left).start()

    def step_b(m):
        gather(m, 0, (z + 3) % 4, 0, right).wait_recv()
        gather(m, 4, (z + 3) % 4, 0, right).start()
        gather(m, 3, (z + 1) % 4, 1, left).wait_recv()
        gather(m, 5, (z + 1) % 4, 1, left).start()

    def step_w(m):
        gather(m, 1, (z + 3) % 4, 1, right).wait_recv()
        gather(m, 2, (z + 1) % 4, 0, left).wait_recv()
        gather(m, 4, far_z, 0, right).wait_recv()
        gather(m, 5, far_z, 1, left).wait_recv()

    xr, xl = device(g, (x + 1) % 4, h, b, z), device(g, (x + 3) % 4, h, b, z)

    def near(way):
        return (x + 1 + 2 * way) % 4

    def half_copy(n, way):
        return remote(
            part.at[n, (x + 2) % 4, way], r1.at[n, way], p1s.at[n, way], p1r.at[n, way], xl if way else xr
        )

    def full_copy(n, way):
        return remote(
            part.at[n, near(way)], r2.at[n, way], p2s.at[n, way], p2r.at[n, way], xl if way else xr
        )

    def pair_copy(n):
        return remote(r2.at[n, 0, 1 - b], yb.at[n], p3s.at[n], p3r.at[n], device(g, x, h, 1 - b, z))

    def step_c(n):
        m, o = n // 2, n % 2
        for bt in range(2):
            product = jnp.dot(
                a[o, bt * half:(bt + 1) * half, :], panel[m], preferred_element_type=F32
            ).astype(BF16)
            for xt in range(4):
                part[n, xt, bt] = product[xt * sl:(xt + 1) * sl]
        half_copy(n, 0).start()
        half_copy(n, 1).start()

    def step_d(n):
        for way in range(2):
            half_copy(n, way).wait_recv()
            part[n, near(way), way] = (
                part[n, near(way), way].astype(F32) + r1[n, way].astype(F32)
            ).astype(BF16)
        for way in range(2):
            full_copy(n, way).start()

    def step_e(n):
        full_copy(n, 0).wait_recv()
        full_copy(n, 1).wait_recv()
        for bt in range(2):
            total = part[n, x, bt].astype(F32) + r2[n, 0, bt].astype(F32) + r2[n, 1, bt].astype(F32)
            r2[n, 0, bt] = total.astype(BF16)

            @pl.when(b == bt)
            def _():
                kept[n] = total

        pair_copy(n).start()

    mine, lanes = aligned(col * sl, sl), aligned(g * H, H)

    def turn(pn, c, o):
        return remote(
            xs.at[pn * 8 + c, o], xst.at[pn, mine, lanes], ts.at[pn, c * 2 + o], tr.at[pn, g * 8 + col],
            ((g + o) % 2, row, c),
        )

    def wait_turned(dst, k):
        def one(i):
            c, gf = (col + i // 2) % 8, (g + i % 2) % 2
            remote(
                xs.at[0, 0], dst.at[aligned(c * sl, sl), aligned(gf * H, H)], ts.at[k, 0], tr.at[k, gf * 8 + c], here
            ).wait_recv()

        loop(1, 16, one)

    def step_f(n):
        m, o = n // 2, n % 2
        pn = n // 8
        pair_copy(n).wait_recv()
        result = (-(kept[n] + yb[n].astype(F32))).astype(BF16)
        for e in range(2):
            xs[2 * m + e, o] = result[:, e * H:(e + 1) * H]
        for e in range(2):
            c = 2 * (m % 4) + e
            self_turn = (c == col) & (o == 0)
            pl.when(jnp.logical_not(self_turn))(turn(pn, c, o).start)

            @pl.when(self_turn)
            def _():
                xst[pn, mine, lanes] = result[:, e * H:(e + 1) * H]

    def pick(i):
        c, o = (col + i // 2) % 8, i % 2
        return remote(
            chosen_s.at[c, o], ct.at[mine, lanes], ts.at[2, i], tr.at[2, g * 8 + col], ((g + o) % 2, row, c)
        )

    def peer(d):
        r = (me + d) % 16
        return r, (r // 8, r % 8, col)

    def scatter(k, d):
        r, to = peer(d)
        return remote(red_s.at[k, r], red.at[k, me], rs.at[k, d], rr.at[k, me], to)

    def reduce_start(k, value):
        red_s[k] = value.reshape(16, B // 16, B).astype(BF16)
        loop(1, 16, lambda d: scatter(k, d).start())
        red[k, me] = red_s[k, me]

    def reduce_end(k):
        def one(d):
            r, _ = peer(d)
            remote(red_s.at[k, r], red.at[k, r], rs.at[k, d], rr.at[k, r], here).wait_recv()

        loop(1, 16, one)
        return jnp.sum(red[k].astype(F32), axis=0)

    outs = (du_out, yp_out, dl_out)

    def spread(k, d):
        r, to = peer(d)
        return remote(outs[k].at[me], outs[k].at[me], gs.at[k, d], gr.at[k, me], to)

    def spread_end(k):
        def one(d):
            r, _ = peer(d)
            remote(outs[k].at[r], outs[k].at[r], gs.at[k, d], gr.at[k, r], here).wait_recv()

        loop(1, 16, one)

    def column(d):
        return remote(dcol.at[col], dcol.at[col], cs.at[d], cr.at[col], (g, row, (col + d) % 8))

    def upper_1():
        for c in range(8):
            chosen_s[c] = xs[parent[c]]
        loop(1, 16, lambda i: pick(i).start())
        ct[mine, lanes] = chosen_s[col, 0]

    def upper_2():
        wait_turned(xst.at[0], 0)
        x_out[...] = xst[0]
        reduce_start(0, flipped(masked[0], xst[0]))
        wait_turned(ct, 2)
        reduce_start(1, flipped(ct[...], masked[1]))
        cl[...] = jnp.dot(ct[...], lp[...], preferred_element_type=F32)

    def upper_3():
        du = (du_in[me] - reduce_end(0)).astype(BF16)
        du_out[me] = du
        dcol[col] = du
        loop(1, 8, lambda d: column(d).start())
        loop(1, 16, lambda d: spread(0, d).start())

    def upper_4():
        crossed = reduce_end(1)

        def one(d):
            c = (col + d) % 8
            remote(dcol.at[c], dcol.at[c], cs.at[d], cr.at[c], here).wait_recv()

        loop(1, 8, one)
        own = dcol[parent[col]]
        yp_out[me] = (-(crossed + jnp.dot(own, lp[...], preferred_element_type=F32))).astype(BF16)
        loop(1, 16, lambda d: spread(1, d).start())

    local_a.wait()
    swap_a.wait_recv()
    step_a(0)
    step_a(1)
    step_b(0)

    def body(n, carry):
        m = n // 2

        @pl.when((n < NS) & (n % 2 == 0))
        def _():
            pl.when(m + 2 < CH)(lambda: step_a(m + 2))
            pl.when(m + 1 < CH)(lambda: step_b(m + 1))
            step_w(m)

        pl.when(n < NS)(lambda: step_c(n))
        for lag, step in ((2, step_d), (4, step_e), (5, step_f)):
            k = n - lag
            pl.when((k >= 0) & (k < NS))(lambda step=step, k=k: step(k))
        for at, step in ((12, upper_1), (14, upper_2), (16, upper_3), (18, upper_4)):
            pl.when(n == at)(step)
        return carry

    lax.fori_loop(0, NS + 5, body, 0)

    wait_turned(xst.at[1], 1)
    y = (xst[1].astype(F32) - cl[...]).astype(BF16)
    y_out[...] = y
    reduce_start(2, flipped(masked[1], y))
    spread_end(1)
    back[...] = flipped(lp[...], yp_out[...].reshape(B, B)).reshape(16, B // 16, B)
    dl_out[me] = (dl_in[me] - reduce_end(2) - back[me]).astype(BF16)
    loop(1, 16, lambda d: spread(2, d).start())

    swap_a.wait_send()
    for pn in range(2):
        for dz, dg in order:
            if (dz, dg) != (0, 0):
                first(pn, dz, dg).wait_send()
        for way in far_first:
            if way != (0, 0, 0):
                second(pn, *way)[2].wait_send()

    def sent_chunk(m):
        for slot in range(6):
            gather(m, slot, z, 0, right).wait_send()

    loop(0, CH, sent_chunk)

    def sent_piece(n):
        for way in range(2):
            half_copy(n, way).wait_send()
            full_copy(n, way).wait_send()
        pair_copy(n).wait_send()

    loop(0, NS, sent_piece)

    def sent_turn(i):
        pick(i).wait_send()
        for pn in range(2):
            turn(pn, (col + i // 2) % 8, i % 2).wait_send()

    loop(1, 16, sent_turn)

    def sent_sum(d):
        for k in range(3):
            scatter(k, d).wait_send()
            spread(k, d).wait_send()

    loop(1, 16, sent_sum)
    loop(1, 8, lambda d: column(d).wait_send())
    spread_end(0)
    spread_end(2)


def step(a, lu, mask_u, du, ll, mask_l, parent, lp, dl):
    rows, depth = a.shape
    quarter, sl, deep = rows // 4, rows // 8, B // 16
    dma = pltpu.SemaphoreType.DMA
    vmem, smem = pl.BlockSpec(memory_space=pltpu.VMEM), pl.BlockSpec(memory_space=pltpu.SMEM)
    block = jax.ShapeDtypeStruct((rows, B), BF16)
    square = jax.ShapeDtypeStruct((16, deep, B), BF16)
    v = pltpu.VMEM
    x, y, d_u, y_p, d_l = pl.pallas_call(
        kernel,
        out_shape=(block, block, square, square, square),
        in_specs=[smem] * 3 + [vmem] * 2 + [pl.BlockSpec(memory_space=pl.ANY)] + [vmem] * 3,
        out_specs=(vmem,) * 5,
        scratch_shapes=[
            v((2, rows, B), BF16),
            v((2, rows, depth), BF16),
            v((2, 4, 2, quarter, H), BF16),
            v((CH, depth, B), BF16),
            v((NS, 4, 2, sl, B), BF16),
            v((NS, 2, sl, B), BF16),
            v((NS, 2, 2, sl, B), BF16),
            v((NS, sl, B), F32),
            v((NS, sl, B), BF16),
            v((16, 2, sl, H), BF16),
            v((8, 2, sl, H), BF16),
            v((2, rows, B), BF16),
            v((rows, B), BF16),
            v((rows, B), F32),
            v((3, 16, deep, B), BF16),
            v((3, 16, deep, B), BF16),
            v((8, deep, B), BF16),
            v((16, deep, B), F32),
            dma, dma, dma,
            dma((2, 8)), dma((2, 8)),
            dma((2, 16)), dma((2, 16)),
            dma((CH, 6)), dma((CH, 6)),
            dma((NS, 2)), dma((NS, 2)),
            dma((NS, 2)), dma((NS, 2)),
            dma((NS,)), dma((NS,)),
            dma((3, 16)), dma((3, 16)),
            dma((3, 16)), dma((3, 16)),
            dma((8,)), dma((8,)),
            dma((3, 16)), dma((3, 16)),
        ],
        compiler_params=pltpu.CompilerParams(has_side_effects=True, vmem_limit_bytes=60 * 2**20),
        name="levels",
    )(mask_u, mask_l, parent, lu, ll, a, lp, du.reshape(16, deep, B), dl.reshape(16, deep, B))
    return x, d_u.reshape(B, B), y, y_p.reshape(B, B), d_l.reshape(B, B)


def solution(mesh):
    rows, cols = P(("grp", "row"), "col"), P(None, "col")
    none = P(None, None)
    return jax.shard_map(
        step,
        mesh=mesh,
        in_specs=(rows, rows, none, cols, rows, none, P(None), cols, cols),
        out_specs=(rows, cols, rows, cols, cols),
        check_vma=False,
    )
```

```python
import jax
import jax.numpy as jnp
from jax import lax
from jax.experimental import pallas as pl
from jax.experimental.pallas import tpu as pltpu
from jax.sharding import PartitionSpec as P

B = 256
H = 128
CH = 8
NS = 16
LAGS = (2, 4, 6)
UPPER = (13, 15)
AHEAD = (2, 1)
ORDER = 2
MESH = pl.DeviceIdType.MESH
F32 = jnp.float32
BF16 = jnp.bfloat16


def device(g, x, h, b, z):
    return (g, z * 2 + h, b * 4 + x)


def swapped(n):
    return n % 2 == 1


def remote(src, dst, send, recv, target):
    return pltpu.make_async_remote_copy(
        src_ref=src, dst_ref=dst, send_sem=send, recv_sem=recv, device_id=target, device_id_type=MESH
    )


def took(ref, sem, target):
    remote(ref, ref, sem, sem, target).wait_recv()


def left_here(ref, sem, target):
    remote(ref, ref, sem, sem, target).wait_send()


def aligned(start, size):
    return pl.ds(pl.multiple_of(start, size), size)


def loop(lo, hi, f):
    def body(i, carry):
        f(i)
        return carry

    lax.fori_loop(lo, hi, body, 0)


def flipped(p, q):
    return lax.dot_general(p, q, (((0,), (0,)), ((), ())), preferred_element_type=F32)


def kernel(
    mask_u_in, mask_l_in, parent_in, lu_in, ll_in, a_in, lp_in, du_arg, dl_arg,
    x_out, y_out, du_out, yp_out, dl_out,
    mask_u, mask_l, parent, lu, ll, lp, du_in, dl_in, masked, a, s1, panel, part, r1, r2, kept, yb, xs, chosen_s, xst, ct, cl, red_s, red, dcol, back,
    in_sem, as_sem, ar_sem, s1s, s1r, s2s, s2r, ags, agr, ps, p1r, p2r, p3r,
    ts, tr, rs, rr, cs, cr, gs, gr,
):
    g, row, col = lax.axis_index("grp"), lax.axis_index("row"), lax.axis_index("col")
    z, h, b, x = row // 2, row % 2, col // 4, col % 4
    me = g * 8 + row
    rows = a.shape[1]
    quarter, sl, half = rows // 4, rows // 8, rows // 2
    bl = min(B, rows)
    here = (g, row, col)

    arrivals_of = ((lu_in, lu), (ll_in, ll), (mask_u_in, mask_u), (mask_l_in, mask_l), (a_in, a.at[0]),
                   (parent_in, parent), (lp_in, lp), (du_arg, du_in), (dl_arg, dl_in))
    loads = [pltpu.make_async_copy(src, dst, in_sem.at[i]) for i, (src, dst) in enumerate(arrivals_of)]
    for load in loads:
        load.start()

    plane = [(0, dx, dy, 0) for dx in range(4) for dy in range(4)]
    line = [(dg, 0, dy, dz) for dg in range(2) for dy in (0, 2) for dz in range(4)]
    across = [(1, dx, db, 0) for dx in range(4) for db in (0, 5)]
    barrier = pltpu.get_barrier_semaphore()
    peers = []
    for dg, dx, dy, dz in plane + line + across:
        if dy == 5:
            key, ht, bt = (dg, dx, 5, dz), h, 1 - b
        else:
            y = (2 * h + b + dy) % 4
            key, ht, bt = (dg, dx, dy, dz), y // 2, y % 2
        if key != (0, 0, 0, 0) and key not in peers:
            peers.append(key)
            pl.semaphore_signal(
                barrier, inc=1, device_id=device((g + dg) % 2, (x + dx) % 4, ht, bt, (z + dz) % 4),
                device_id_type=MESH,
            )

    for load in loads[:4]:
        load.wait()
    for pn, (factor, mask) in enumerate(((lu, mask_u), (ll, mask_l))):
        for i in range(rows // bl):
            keep = mask[col, (me * rows + i * bl) // B] > 0
            values = factor[i * bl:(i + 1) * bl, :]
            masked[pn, i * bl:(i + 1) * bl, :] = jnp.where(keep, values, jnp.zeros_like(values))

    swap_a = remote(a.at[0], a.at[1], as_sem, ar_sem, (1 - g, row, col))
    pl.semaphore_wait(barrier, len(peers))

    def piece(pn, q, half_of):
        return masked.at[pn, aligned(q * quarter, quarter), aligned(half_of * H, H)]

    def first(pn, dz, dg):
        gt, zt = (g + dg) % 2, (z + dz) % 4
        return remote(
            piece(pn, zt, gt), s1.at[g, z, pn], s1s.at[pn], s1r.at[pn, g * 4 + z],
            device(gt, x, h, b, zt),
        )

    def first_in(pn, dz, dg):
        gf, zf = (g + dg) % 2, (z + dz) % 4
        return remote(piece(pn, z, g), s1.at[gf, zf, pn], s1s.at[pn], s1r.at[pn, gf * 4 + zf], here)

    order = [(dz, dg) for dz in (2, 1, 3, 0) for dg in (0, 1)]
    for pn in range(2):
        for dz, dg in order:
            if (dz, dg) != (0, 0):
                first(pn, dz, dg).start()
        s1[g, z, pn] = masked[pn, aligned(z * quarter, quarter), aligned(g * H, H)]

    def spot_from(pn, hf, cf, lane):
        return (pn * 4 + cf // 2, aligned(hf * rows + z * quarter, quarter), lane)

    def second(pn, dz, dg, dh):
        zf, gf, ht = (z + dz) % 4, (g + dg) % 2, (h + dh) % 2
        stays = (zf == x) & (gf == b) & (ht == h)
        return stays, zf, gf, remote(
            s1.at[gf, zf, pn], panel.at[spot_from(pn, h, col, aligned((col % 2) * H, H))],
            s2s.at[pn], s2r.at[pn * 4 + col // 2], device(g, zf, ht, gf, z),
        )

    arrivals = [(dz, dg) for dz in (0, 1, 3, 2) for dg in (0, 1)]
    def pass_on(pn):
        for dz, dg in arrivals:
            if (dz, dg) != (0, 0):
                first_in(pn, dz, dg).wait_recv()
            for dh in range(2):
                stays, zf, gf, copy = second(pn, dz, dg, dh)
                pl.when(jnp.logical_not(stays))(copy.start)

                @pl.when(stays)
                def _(zf=zf, gf=gf):
                    panel[spot_from(pn, h, col, aligned((col % 2) * H, H))] = s1[gf, zf, pn]

    pass_on(0)
    loads[4].wait()
    swap_a.start()

    right, left = device(g, x, h, b, (z + 1) % 4), device(g, x, h, b, (z + 3) % 4)

    def gather(m, kind, q, hf, to):
        spot = panel.at[m, aligned(hf * rows + q * quarter, quarter)]
        return remote(spot, spot, ags, agr.at[m, kind], to)

    def step_a(m):
        own = col // 2 == m % 4
        pl.when(own)(lambda: took(panel.at[m, pl.ds(0, 3 * quarter // 2)], s2r.at[m], here))
        pl.when(jnp.logical_not(own))(lambda: took(panel.at[m, pl.ds(0, 2 * quarter)], s2r.at[m], here))
        gather(m, 0, z, 0, right).start()
        gather(m, 1, z, 1, left).start()
        gather(m, 2, z, 1, right).start()
        gather(m, 2, z, 0, left).start()

    def step_b(m):
        gather(m, 0, (z + 3) % 4, 0, right).wait_recv()
        gather(m, 2, (z + 3) % 4, 0, right).start()
        gather(m, 1, (z + 1) % 4, 1, left).wait_recv()
        gather(m, 2, (z + 1) % 4, 1, left).start()

    def step_w(m):
        took(panel.at[m, pl.ds(0, rows)], agr.at[m, 2], here)

    xr, xl = device(g, (x + 1) % 4, h, b, z), device(g, (x + 3) % 4, h, b, z)
    yp = device(g, x, h, 1 - b, z)
    far_x = (x + 2) % 4
    low = sl // 2

    def near(way):
        return (x + 1 + 2 * way) % 4

    def x_copy(src, dst, arrived, way):
        return remote(src, dst, ps, arrived, xl if way else xr)

    def half_even(n, way):
        return x_copy(part.at[n, way, far_x], r1.at[n, way], p1r.at[n], way)

    def half_odd(n, way):
        return x_copy(part.at[n, b, far_x, pl.ds(way * low, low)], r1.at[n, 0, pl.ds(way * low, low)], p1r.at[n], way)

    def full_even(n, way):
        return x_copy(part.at[n, :, near(way)], r2.at[n, way], p2r.at[n], way)

    def full_odd(n, way):
        return x_copy(part.at[n, b, near(way)], r2.at[n, 0, way], p2r.at[n], way)

    def pair_even(n):
        return remote(r2.at[n, 0, 1 - b], yb.at[n, 0], ps, p3r.at[n], yp)

    def pair_odd(n):
        return remote(part.at[n, 1 - b], yb.at[n], ps, p3r.at[n], yp)

    def add(p, q):
        return (p.astype(F32) + q.astype(F32)).astype(BF16)

    def by_parity(n, even, odd):
        pl.when(jnp.logical_not(swapped(n)))(lambda: even(n))
        pl.when(swapped(n))(lambda: odd(n))

    def step_c(n):
        m, o = n // 2, n % 2
        for bt in range(2):
            product = jnp.dot(
                a[o, bt * half:(bt + 1) * half, :], panel[m], preferred_element_type=F32
            ).astype(BF16)
            for xt in range(4):
                part[n, bt, xt] = product[xt * sl:(xt + 1) * sl]

        def even(n):
            half_even(n, 0).start()
            half_even(n, 1).start()

        by_parity(n, even, lambda n: pair_odd(n).start())

    def step_d(n):
        def even(n):
            took(r1.at[n], p1r.at[n], here)
            for way in range(2):
                part[n, way, near(way)] = add(part[n, way, near(way)], r1[n, way])
            full_even(n, 0).start()
            full_even(n, 1).start()

        def odd(n):
            pair_odd(n).wait_recv()
            for xt in range(4):
                part[n, b, xt] = add(part[n, b, xt], yb[n, xt])
            half_odd(n, 0).start()
            half_odd(n, 1).start()

        by_parity(n, even, odd)

    def step_e(n):
        def even(n):
            took(r2.at[n], p2r.at[n], here)
            for bt in range(2):
                total = part[n, bt, x].astype(F32) + r2[n, 0, bt].astype(F32) + r2[n, 1, bt].astype(F32)
                r2[n, 0, bt] = total.astype(BF16)

                @pl.when(b == bt)
                def _():
                    kept[n] = total

            pair_even(n).start()

        def odd(n):
            took(r1.at[n, 0], p1r.at[n], here)
            for way in range(2):
                spot = (n, b, near(way), pl.ds(way * low, low))
                part[spot] = add(part[spot], r1[n, 0, way * low:(way + 1) * low])
            full_odd(n, 0).start()
            full_odd(n, 1).start()

        by_parity(n, even, odd)

    def finish(n):
        def even(n):
            pair_even(n).wait_recv()
            kept[n] = -(kept[n] + yb[n, 0].astype(F32))

        def odd(n):
            took(r2.at[n, 0], p2r.at[n], here)
            kept[n] = -(part[n, b, x].astype(F32) + r2[n, 0, 0].astype(F32) + r2[n, 0, 1].astype(F32))

        by_parity(n, even, odd)
        return kept[n].astype(BF16)

    mine, lanes = aligned(col * sl, sl), aligned(g * H, H)

    def turn(pn, c, o):
        return remote(
            xs.at[pn * 8 + c, o], xst.at[pn, mine, lanes], ts.at[pn], tr.at[pn],
            ((g + o) % 2, row, c),
        )

    def wait_turned(dst, k):
        took(dst.at[pl.ds(0, 15 * sl // 2)], tr.at[k], here)

    def step_f(n):
        m, o = n // 2, n % 2
        pn = n // 8
        result = finish(n)
        for e in range(2):
            xs[2 * m + e, o] = result[:, e * H:(e + 1) * H]
        for e in range(2):
            c = 2 * (m % 4) + e
            self_turn = (c == col) & (o == 0)
            pl.when(jnp.logical_not(self_turn))(turn(pn, c, o).start)

            @pl.when(self_turn)
            def _():
                xst[pn, mine, lanes] = result[:, e * H:(e + 1) * H]

    def pick(i):
        c, o = (col + i // 2) % 8, i % 2
        return remote(
            chosen_s.at[c, o], ct.at[mine, lanes], ts.at[2], tr.at[2], ((g + o) % 2, row, c)
        )

    def peer(d):
        r = (me + d) % 16
        return r, (r // 8, r % 8, col)

    def scatter(k, d):
        r, to = peer(d)
        return remote(red_s.at[k, r], red.at[k, me], rs.at[k], rr.at[k], to)

    def reduce_start(k, value):
        red_s[k] = value.reshape(16, B // 16, B).astype(BF16)
        loop(1, 16, lambda d: scatter(k, d).start())
        red[k, me] = red_s[k, me]

    def reduce_end(k):
        took(red.at[k, pl.ds(0, 15)], rr.at[k], here)
        return jnp.sum(red[k].astype(F32), axis=0)

    outs = (du_out, yp_out, dl_out)

    def spread(k, d):
        r, to = peer(d)
        return remote(outs[k].at[me], outs[k].at[me], gs.at[k], gr.at[k], to)

    def spread_end(k):
        took(outs[k].at[pl.ds(0, 15)], gr.at[k], here)

    def column(d):
        return remote(dcol.at[col], dcol.at[col], cs, cr, (g, row, (col + d) % 8))

    def upper_1():
        for c in range(8):
            chosen_s[c] = xs[parent[c]]
        loop(1, 16, lambda i: pick(i).start())
        ct[mine, lanes] = chosen_s[col, 0]

    def upper_2():
        wait_turned(xst.at[0], 0)
        x_out[...] = xst[0]
        reduce_start(0, flipped(masked[0], xst[0]))
        wait_turned(ct, 2)
        reduce_start(1, flipped(ct[...], masked[1]))
        cl[...] = jnp.dot(ct[...], lp[...], preferred_element_type=F32)

    def upper_3():
        du = (du_in[me] - reduce_end(0)).astype(BF16)
        du_out[me] = du
        dcol[col] = du
        loop(1, 8, lambda d: column(d).start())
        loop(1, 16, lambda d: spread(0, d).start())

    def upper_4():
        crossed = reduce_end(1)
        took(dcol.at[pl.ds(0, 7)], cr, here)
        own = dcol[parent[col]]
        yp_out[me] = (-(crossed + jnp.dot(own, lp[...], preferred_element_type=F32))).astype(BF16)
        loop(1, 16, lambda d: spread(1, d).start())

    for load in loads[5:]:
        load.wait()
    if ORDER == 0:
        pass_on(1)
    for m in range(AHEAD[0]):
        step_a(m)
    if ORDER == 1:
        pass_on(1)
    for m in range(AHEAD[1]):
        step_b(m)
    if ORDER == 2:
        pass_on(1)
    swap_a.wait_recv()

    def body(n, carry):
        m = n // 2

        @pl.when((n < NS) & (n % 2 == 0))
        def _():
            pl.when(m + AHEAD[0] < CH)(lambda: step_a(m + AHEAD[0]))
            pl.when(m + AHEAD[1] < CH)(lambda: step_b(m + AHEAD[1]))
            step_w(m)

        pl.when(n < NS)(lambda: step_c(n))
        for lag, step in zip(LAGS, (step_d, step_e, step_f)):
            k = n - lag
            pl.when((k >= 0) & (k < NS))(lambda step=step, k=k: step(k))
        for at, step in zip(UPPER, (upper_1, upper_2)):
            pl.when(n == at)(step)
        return carry

    lax.fori_loop(0, NS + LAGS[-1], body, 0)

    upper_3()
    wait_turned(xst.at[1], 1)
    y = (xst[1].astype(F32) - cl[...]).astype(BF16)
    y_out[...] = y
    reduce_start(2, flipped(masked[1], y))
    upper_4()
    lower = dl_in[me] - reduce_end(2)
    spread_end(1)
    back[...] = flipped(lp[...], yp_out[...].reshape(B, B)).reshape(16, B // 16, B)
    dl_out[me] = (lower - back[me]).astype(BF16)
    loop(1, 16, lambda d: spread(2, d).start())

    swap_a.wait_send()
    for pn in range(2):
        left_here(panel.at[0, pl.ds(0, 7 * quarter // 2)], s1s.at[pn], here)
        left_here(panel.at[0, pl.ds(0, 15 * quarter // 2)], s2s.at[pn], here)
    left_here(panel.at[pl.ds(0, 6)], ags, here)
    left_here(panel.at[pl.ds(0, 7)], ps, here)
    for k in range(3):
        left_here(ct.at[pl.ds(0, 15 * sl // 2)], ts.at[k], here)
        left_here(red_s.at[k, pl.ds(0, 15)], rs.at[k], here)
        left_here(outs[k].at[pl.ds(0, 15)], gs.at[k], here)
    left_here(dcol.at[pl.ds(0, 7)], cs, here)
    spread_end(0)
    spread_end(2)


def step(a, lu, mask_u, du, ll, mask_l, parent, lp, dl):
    rows, depth = a.shape
    quarter, sl, deep = rows // 4, rows // 8, B // 16
    dma = pltpu.SemaphoreType.DMA
    vmem = pl.BlockSpec(memory_space=pltpu.VMEM)
    block = jax.ShapeDtypeStruct((rows, B), BF16)
    square = jax.ShapeDtypeStruct((16, deep, B), BF16)
    v = pltpu.VMEM
    x, y, d_u, y_p, d_l = pl.pallas_call(
        kernel,
        out_shape=(block, block, square, square, square),
        in_specs=[pl.BlockSpec(memory_space=pltpu.HBM)] * 9,
        out_specs=(vmem,) * 5,
        scratch_shapes=[
            pltpu.SMEM(mask_u.shape, jnp.int32),
            pltpu.SMEM(mask_l.shape, jnp.int32),
            pltpu.SMEM(parent.shape, jnp.int32),
            v((rows, B), BF16),
            v((rows, B), BF16),
            v((B, B), BF16),
            v((16, deep, B), F32),
            v((16, deep, B), F32),
            v((2, rows, B), BF16),
            v((2, rows, depth), BF16),
            v((2, 4, 2, quarter, H), BF16),
            v((CH, depth, B), BF16),
            v((NS, 2, 4, sl, B), BF16),
            v((NS, 2, sl, B), BF16),
            v((NS, 2, 2, sl, B), BF16),
            v((NS, sl, B), F32),
            v((NS, 4, sl, B), BF16),
            v((16, 2, sl, H), BF16),
            v((8, 2, sl, H), BF16),
            v((2, rows, B), BF16),
            v((rows, B), BF16),
            v((rows, B), F32),
            v((3, 16, deep, B), BF16),
            v((3, 16, deep, B), BF16),
            v((8, deep, B), BF16),
            v((16, deep, B), F32),
            dma((9,)), dma, dma,
            dma((2,)), dma((2, 8)),
            dma((2,)), dma((CH,)),
            dma, dma((CH, 3)),
            dma, dma((NS,)), dma((NS,)), dma((NS,)),
            dma((3,)), dma((3,)),
            dma((3,)), dma((3,)),
            dma, dma,
            dma((3,)), dma((3,)),
        ],
        compiler_params=pltpu.CompilerParams(collective_id=0, has_side_effects=True, vmem_limit_bytes=60 * 2**20),
        name="levels",
    )(mask_u, mask_l, parent, lu, ll, a, lp, du.reshape(16, deep, B), dl.reshape(16, deep, B))
    return place((x, d_u.reshape(B, B), y, y_p.reshape(B, B), d_l.reshape(B, B)))


def place_kernel(*refs):
    n = (len(refs) - 2) // 3
    sources, outs, held, sems_in, sems_out = refs[:n], refs[n:2 * n], refs[2 * n:3 * n], refs[-2], refs[-1]
    ins = [pltpu.make_async_copy(sources[i], held[i], sems_in.at[i]) for i in range(n)]
    puts = [pltpu.make_async_copy(held[i], outs[i], sems_out.at[i]) for i in range(n)]
    for copy in ins:
        copy.start()
    for i in range(n):
        ins[i].wait()
        puts[i].start()
    for copy in puts:
        copy.wait()


def place(arrays):
    n = len(arrays)
    hbm = pl.BlockSpec(memory_space=pltpu.HBM)
    return pl.pallas_call(
        place_kernel,
        out_shape=tuple(jax.ShapeDtypeStruct(v.shape, v.dtype) for v in arrays),
        in_specs=[hbm] * n,
        out_specs=(hbm,) * n,
        scratch_shapes=[pltpu.VMEM(v.shape, v.dtype) for v in arrays]
        + [pltpu.SemaphoreType.DMA((n,)), pltpu.SemaphoreType.DMA((n,))],
        compiler_params=pltpu.CompilerParams(vmem_limit_bytes=60 * 2**20),
        name="place",
    )(*arrays)


def solution(mesh):
    rows, cols = P(("grp", "row"), "col"), P(None, "col")
    none = P(None, None)
    return jax.shard_map(
        step,
        mesh=mesh,
        in_specs=(rows, rows, none, cols, rows, none, P(None), cols, cols),
        out_specs=(rows, cols, rows, cols, cols),
        check_vma=False,
    )
```

```python
import jax
import jax.numpy as jnp
from jax import lax
from jax.experimental import pallas as pl
from jax.experimental.pallas import tpu as pltpu
from jax.sharding import PartitionSpec as P

B = 256
H = 128
CH = 8
NS = 16
LAGS = (2, 4, 6)
UPPER = (13, 15, 19)
AHEAD = (2, 1)
MESH = pl.DeviceIdType.MESH
F32 = jnp.float32
BF16 = jnp.bfloat16


def device(g, x, h, b, z):
    return (g, z * 2 + h, b * 4 + x)


def swapped(n):
    return n % 2 == 1


def remote(src, dst, send, recv, target):
    return pltpu.make_async_remote_copy(
        src_ref=src, dst_ref=dst, send_sem=send, recv_sem=recv, device_id=target, device_id_type=MESH
    )


def took(ref, sem, target):
    remote(ref, ref, sem, sem, target).wait_recv()


def left_here(ref, sem, target):
    remote(ref, ref, sem, sem, target).wait_send()


def aligned(start, size):
    return pl.ds(pl.multiple_of(start, size), size)


def loop(lo, hi, f):
    def body(i, carry):
        f(i)
        return carry

    lax.fori_loop(lo, hi, body, 0)


def flipped(p, q):
    return lax.dot_general(p, q, (((0,), (0,)), ((), ())), preferred_element_type=F32)


def kernel(
    mask_u_in, mask_l_in, parent_in, lu_in, ll_in, a_in, lp_in, du_arg, dl_arg,
    x_out, y_out, du_out, yp_out, dl_out,
    mask_u, mask_l, parent, lu, ll, lp, du_in, dl_in, masked, a, s1, panel, part, r1, r2, kept, yb, xs, chosen_s, xst, ct, cl, red_s, red, dcol, back, y_held, du_held, yp_held, dl_held,
    in_sem, out_sem, as_sem, ar_sem, s1s, s1r, s2s, s2r, ags, agr, ps, p1r, p2r, p3r,
    ts, tr, rs, rr, cs, cr, gs, gr,
):
    g, row, col = lax.axis_index("grp"), lax.axis_index("row"), lax.axis_index("col")
    z, h, b, x = row // 2, row % 2, col // 4, col % 4
    me = g * 8 + row
    rows = a.shape[1]
    quarter, sl, half = rows // 4, rows // 8, rows // 2
    bl = min(B, rows)
    here = (g, row, col)

    arrivals_of = ((lu_in, lu), (ll_in, ll), (mask_u_in, mask_u), (mask_l_in, mask_l), (a_in, a.at[0]),
                   (parent_in, parent), (lp_in, lp), (du_arg, du_in), (dl_arg, dl_in))
    loads = [pltpu.make_async_copy(src, dst, in_sem.at[i]) for i, (src, dst) in enumerate(arrivals_of)]
    for load in loads:
        load.start()

    plane = [(0, dx, dy, 0) for dx in range(4) for dy in range(4)]
    line = [(dg, 0, dy, dz) for dg in range(2) for dy in (0, 2) for dz in range(4)]
    across = [(1, dx, db, 0) for dx in range(4) for db in (0, 5)]
    barrier = pltpu.get_barrier_semaphore()
    peers = []
    for dg, dx, dy, dz in plane + line + across:
        if dy == 5:
            key, ht, bt = (dg, dx, 5, dz), h, 1 - b
        else:
            y = (2 * h + b + dy) % 4
            key, ht, bt = (dg, dx, dy, dz), y // 2, y % 2
        if key != (0, 0, 0, 0) and key not in peers:
            peers.append(key)
            pl.semaphore_signal(
                barrier, inc=1, device_id=device((g + dg) % 2, (x + dx) % 4, ht, bt, (z + dz) % 4),
                device_id_type=MESH,
            )

    for load in loads[:4]:
        load.wait()
    for pn, (factor, mask) in enumerate(((lu, mask_u), (ll, mask_l))):
        for i in range(rows // bl):
            keep = mask[col, (me * rows + i * bl) // B] > 0
            values = factor[i * bl:(i + 1) * bl, :]
            masked[pn, i * bl:(i + 1) * bl, :] = jnp.where(keep, values, jnp.zeros_like(values))

    swap_a = remote(a.at[0], a.at[1], as_sem, ar_sem, (1 - g, row, col))
    pl.semaphore_wait(barrier, len(peers))

    def piece(pn, q, half_of):
        return masked.at[pn, aligned(q * quarter, quarter), aligned(half_of * H, H)]

    def first(pn, dz, dg):
        gt, zt = (g + dg) % 2, (z + dz) % 4
        return remote(
            piece(pn, zt, gt), s1.at[g, z, pn], s1s.at[pn], s1r.at[pn, g * 4 + z],
            device(gt, x, h, b, zt),
        )

    def first_in(pn, dz, dg):
        gf, zf = (g + dg) % 2, (z + dz) % 4
        return remote(piece(pn, z, g), s1.at[gf, zf, pn], s1s.at[pn], s1r.at[pn, gf * 4 + zf], here)

    order = [(dz, dg) for dz in (2, 1, 3, 0) for dg in (0, 1)]
    def hand_out(pn):
        for dz, dg in order:
            if (dz, dg) != (0, 0):
                first(pn, dz, dg).start()
        s1[g, z, pn] = masked[pn, aligned(z * quarter, quarter), aligned(g * H, H)]

    hand_out(0)
    hand_out(1)

    def spot_from(pn, hf, cf, lane):
        return (pn * 4 + cf // 2, aligned(hf * rows + z * quarter, quarter), lane)

    def second(pn, dz, dg, dh):
        zf, gf, ht = (z + dz) % 4, (g + dg) % 2, (h + dh) % 2
        stays = (zf == x) & (gf == b) & (ht == h)
        return stays, zf, gf, remote(
            s1.at[gf, zf, pn], panel.at[spot_from(pn, h, col, aligned((col % 2) * H, H))],
            s2s.at[pn], s2r.at[pn * 4 + col // 2], device(g, zf, ht, gf, z),
        )

    arrivals = [(dz, dg) for dz in (0, 1, 3, 2) for dg in (0, 1)]
    def pass_on(pn):
        for dz, dg in arrivals:
            if (dz, dg) != (0, 0):
                first_in(pn, dz, dg).wait_recv()
            for dh in range(2):
                stays, zf, gf, copy = second(pn, dz, dg, dh)
                pl.when(jnp.logical_not(stays))(copy.start)

                @pl.when(stays)
                def _(zf=zf, gf=gf):
                    panel[spot_from(pn, h, col, aligned((col % 2) * H, H))] = s1[gf, zf, pn]

    pass_on(0)
    loads[4].wait()
    swap_a.start()

    right, left = device(g, x, h, b, (z + 1) % 4), device(g, x, h, b, (z + 3) % 4)

    def gather(m, kind, q, hf, to):
        spot = panel.at[m, aligned(hf * rows + q * quarter, quarter)]
        return remote(spot, spot, ags, agr.at[m, kind], to)

    def step_a(m):
        own = col // 2 == m % 4
        pl.when(own)(lambda: took(panel.at[m, pl.ds(0, 3 * quarter // 2)], s2r.at[m], here))
        pl.when(jnp.logical_not(own))(lambda: took(panel.at[m, pl.ds(0, 2 * quarter)], s2r.at[m], here))
        gather(m, 0, z, 0, right).start()
        gather(m, 1, z, 1, left).start()
        gather(m, 2, z, 1, right).start()
        gather(m, 2, z, 0, left).start()

    def step_b(m):
        gather(m, 0, (z + 3) % 4, 0, right).wait_recv()
        gather(m, 2, (z + 3) % 4, 0, right).start()
        gather(m, 1, (z + 1) % 4, 1, left).wait_recv()
        gather(m, 2, (z + 1) % 4, 1, left).start()

    def step_w(m):
        took(panel.at[m, pl.ds(0, rows)], agr.at[m, 2], here)

    xr, xl = device(g, (x + 1) % 4, h, b, z), device(g, (x + 3) % 4, h, b, z)
    yp = device(g, x, h, 1 - b, z)
    far_x = (x + 2) % 4
    low = sl // 2

    def near(way):
        return (x + 1 + 2 * way) % 4

    def x_copy(src, dst, arrived, way):
        return remote(src, dst, ps, arrived, xl if way else xr)

    def half_even(n, way):
        return x_copy(part.at[n, way, far_x], r1.at[n, way], p1r.at[n], way)

    def half_odd(n, way):
        return x_copy(part.at[n, b, far_x, pl.ds(way * low, low)], r1.at[n, 0, pl.ds(way * low, low)], p1r.at[n], way)

    def full_even(n, way):
        return x_copy(part.at[n, :, near(way)], r2.at[n, way], p2r.at[n], way)

    def full_odd(n, way):
        return x_copy(part.at[n, b, near(way)], r2.at[n, 0, way], p2r.at[n], way)

    def pair_even(n):
        return remote(r2.at[n, 0, 1 - b], yb.at[n, 0], ps, p3r.at[n], yp)

    def pair_odd(n):
        return remote(part.at[n, 1 - b], yb.at[n], ps, p3r.at[n], yp)

    def add(p, q):
        return (p.astype(F32) + q.astype(F32)).astype(BF16)

    def by_parity(n, even, odd):
        pl.when(jnp.logical_not(swapped(n)))(lambda: even(n))
        pl.when(swapped(n))(lambda: odd(n))

    def step_c(n):
        m, o = n // 2, n % 2
        for bt in range(2):
            product = jnp.dot(
                a[o, bt * half:(bt + 1) * half, :], panel[m], preferred_element_type=F32
            ).astype(BF16)
            for xt in range(4):
                part[n, bt, xt] = product[xt * sl:(xt + 1) * sl]

        def even(n):
            half_even(n, 0).start()
            half_even(n, 1).start()

        by_parity(n, even, lambda n: pair_odd(n).start())

    def step_d(n):
        def even(n):
            took(r1.at[n], p1r.at[n], here)
            for way in range(2):
                part[n, way, near(way)] = add(part[n, way, near(way)], r1[n, way])
            full_even(n, 0).start()
            full_even(n, 1).start()

        def odd(n):
            pair_odd(n).wait_recv()
            for xt in range(4):
                part[n, b, xt] = add(part[n, b, xt], yb[n, xt])
            half_odd(n, 0).start()
            half_odd(n, 1).start()

        by_parity(n, even, odd)

    def step_e(n):
        def even(n):
            took(r2.at[n], p2r.at[n], here)
            for bt in range(2):
                total = part[n, bt, x].astype(F32) + r2[n, 0, bt].astype(F32) + r2[n, 1, bt].astype(F32)
                r2[n, 0, bt] = total.astype(BF16)

                @pl.when(b == bt)
                def _():
                    kept[n] = total

            pair_even(n).start()

        def odd(n):
            took(r1.at[n, 0], p1r.at[n], here)
            for way in range(2):
                spot = (n, b, near(way), pl.ds(way * low, low))
                part[spot] = add(part[spot], r1[n, 0, way * low:(way + 1) * low])
            full_odd(n, 0).start()
            full_odd(n, 1).start()

        by_parity(n, even, odd)

    def finish(n):
        def even(n):
            pair_even(n).wait_recv()
            kept[n] = -(kept[n] + yb[n, 0].astype(F32))

        def odd(n):
            took(r2.at[n, 0], p2r.at[n], here)
            kept[n] = -(part[n, b, x].astype(F32) + r2[n, 0, 0].astype(F32) + r2[n, 0, 1].astype(F32))

        by_parity(n, even, odd)
        return kept[n].astype(BF16)

    mine, lanes = aligned(col * sl, sl), aligned(g * H, H)

    def turn(pn, c, o):
        return remote(
            xs.at[pn * 8 + c, o], xst.at[pn, mine, lanes], ts.at[pn], tr.at[pn],
            ((g + o) % 2, row, c),
        )

    def wait_turned(dst, k):
        took(dst.at[pl.ds(0, 15 * sl // 2)], tr.at[k], here)

    def step_f(n):
        m, o = n // 2, n % 2
        pn = n // 8
        result = finish(n)
        for e in range(2):
            xs[2 * m + e, o] = result[:, e * H:(e + 1) * H]
        for e in range(2):
            c = 2 * (m % 4) + e
            self_turn = (c == col) & (o == 0)
            pl.when(jnp.logical_not(self_turn))(turn(pn, c, o).start)

            @pl.when(self_turn)
            def _():
                xst[pn, mine, lanes] = result[:, e * H:(e + 1) * H]

    def pick(i):
        c, o = (col + i // 2) % 8, i % 2
        return remote(
            chosen_s.at[c, o], ct.at[mine, lanes], ts.at[2], tr.at[2], ((g + o) % 2, row, c)
        )

    def peer(d):
        r = (me + d) % 16
        return r, (r // 8, r % 8, col)

    def scatter(k, d):
        r, to = peer(d)
        return remote(red_s.at[k, r], red.at[k, me], rs.at[k], rr.at[k], to)

    def reduce_start(k, value):
        red_s[k] = value.reshape(16, B // 16, B).astype(BF16)
        loop(1, 16, lambda d: scatter(k, d).start())
        red[k, me] = red_s[k, me]

    def reduce_end(k):
        took(red.at[k, pl.ds(0, 15)], rr.at[k], here)
        return jnp.sum(red[k].astype(F32), axis=0)

    outs = (du_held, yp_held, dl_held)
    x_put, y_put, du_put, yp_put, dl_put = [
        pltpu.make_async_copy(src, dst, out_sem.at[i])
        for i, (src, dst) in enumerate(
            ((xst.at[0], x_out), (y_held, y_out), (du_held, du_out), (yp_held, yp_out), (dl_held, dl_out))
        )
    ]

    def spread(k, d):
        r, to = peer(d)
        return remote(outs[k].at[me], outs[k].at[me], gs.at[k], gr.at[k], to)

    def spread_end(k):
        took(outs[k].at[pl.ds(0, 15)], gr.at[k], here)

    def column(d):
        return remote(dcol.at[col], dcol.at[col], cs, cr, (g, row, (col + d) % 8))

    def upper_1():
        for c in range(8):
            chosen_s[c] = xs[parent[c]]
        loop(1, 16, lambda i: pick(i).start())
        ct[mine, lanes] = chosen_s[col, 0]

    def upper_2():
        wait_turned(xst.at[0], 0)
        x_put.start()
        reduce_start(0, flipped(masked[0], xst[0]))
        wait_turned(ct, 2)
        reduce_start(1, flipped(ct[...], masked[1]))
        cl[...] = jnp.dot(ct[...], lp[...], preferred_element_type=F32)

    def upper_3():
        du = (du_in[me] - reduce_end(0)).astype(BF16)
        du_held[me] = du
        dcol[col] = du
        loop(1, 8, lambda d: column(d).start())
        loop(1, 16, lambda d: spread(0, d).start())

    def upper_4():
        crossed = reduce_end(1)
        took(dcol.at[pl.ds(0, 7)], cr, here)
        own = dcol[parent[col]]
        held = (-(crossed + jnp.dot(own, lp[...], preferred_element_type=F32))).astype(BF16)
        yp_held[me] = held
        loop(1, 16, lambda d: spread(1, d).start())
        back[...] = flipped(lp[aligned(me * (B // 16), B // 16), :], held)

    for load in loads[5:]:
        load.wait()
    step_a(0)
    step_a(1)
    step_b(0)
    pass_on(1)
    swap_a.wait_recv()

    def body(n, carry):
        m = n // 2
        starts = (n < NS) & (n % 2 == 0)

        def late():
            for lag, step in zip(LAGS, (step_d, step_e, step_f)):
                k = n - lag
                pl.when((k >= 0) & (k < NS))(lambda step=step, k=k: step(k))
            for at, step in zip(UPPER, (upper_1, upper_2, upper_3)):
                pl.when(n == at)(step)

        @pl.when(starts)
        def _():
            pl.when(m + AHEAD[0] < CH)(lambda: step_a(m + AHEAD[0]))
            pl.when(m + AHEAD[1] < CH)(lambda: step_b(m + AHEAD[1]))

        pl.when(starts)(lambda: step_w(m))
        pl.when(n < NS)(lambda: step_c(n))
        late()
        return carry

    lax.fori_loop(0, NS + LAGS[-1], body, 0)

    upper_4()
    wait_turned(xst.at[1], 1)
    y = (xst[1].astype(F32) - cl[...]).astype(BF16)
    y_held[...] = y
    y_put.start()
    reduce_start(2, flipped(masked[1], y) + back[...])
    dl_held[me] = (dl_in[me] - reduce_end(2)).astype(BF16)
    loop(1, 16, lambda d: spread(2, d).start())
    spread_end(0)
    du_put.start()
    spread_end(1)
    yp_put.start()

    swap_a.wait_send()
    for pn in range(2):
        left_here(panel.at[0, pl.ds(0, 7 * quarter // 2)], s1s.at[pn], here)
        left_here(panel.at[0, pl.ds(0, 15 * quarter // 2)], s2s.at[pn], here)
    left_here(panel.at[pl.ds(0, 6)], ags, here)
    left_here(panel.at[pl.ds(0, 7)], ps, here)
    for k in range(3):
        left_here(ct.at[pl.ds(0, 15 * sl // 2)], ts.at[k], here)
        left_here(red_s.at[k, pl.ds(0, 15)], rs.at[k], here)
        left_here(outs[k].at[pl.ds(0, 15)], gs.at[k], here)
    left_here(dcol.at[pl.ds(0, 7)], cs, here)
    spread_end(2)
    dl_put.start()
    for put in (x_put, y_put, du_put, yp_put, dl_put):
        put.wait()


def step(a, lu, mask_u, du, ll, mask_l, parent, lp, dl):
    rows, depth = a.shape
    quarter, sl, deep = rows // 4, rows // 8, B // 16
    dma = pltpu.SemaphoreType.DMA
    block = jax.ShapeDtypeStruct((rows, B), BF16)
    square = jax.ShapeDtypeStruct((16, deep, B), BF16)
    v = pltpu.VMEM
    x, y, d_u, y_p, d_l = pl.pallas_call(
        kernel,
        out_shape=(block, block, square, square, square),
        in_specs=[pl.BlockSpec(memory_space=pltpu.HBM)] * 9,
        out_specs=(pl.BlockSpec(memory_space=pltpu.HBM),) * 5,
        scratch_shapes=[
            pltpu.SMEM(mask_u.shape, jnp.int32),
            pltpu.SMEM(mask_l.shape, jnp.int32),
            pltpu.SMEM(parent.shape, jnp.int32),
            v((rows, B), BF16),
            v((rows, B), BF16),
            v((B, B), BF16),
            v((16, deep, B), F32),
            v((16, deep, B), F32),
            v((2, rows, B), BF16),
            v((2, rows, depth), BF16),
            v((2, 4, 2, quarter, H), BF16),
            v((CH, depth, B), BF16),
            v((NS, 2, 4, sl, B), BF16),
            v((NS, 2, sl, B), BF16),
            v((NS, 2, 2, sl, B), BF16),
            v((NS, sl, B), F32),
            v((NS, 4, sl, B), BF16),
            v((16, 2, sl, H), BF16),
            v((8, 2, sl, H), BF16),
            v((2, rows, B), BF16),
            v((rows, B), BF16),
            v((rows, B), F32),
            v((3, 16, deep, B), BF16),
            v((3, 16, deep, B), BF16),
            v((8, deep, B), BF16),
            v((B, B), F32),
            v((rows, B), BF16),
            v((16, deep, B), BF16),
            v((16, deep, B), BF16),
            v((16, deep, B), BF16),
            dma((9,)), dma((5,)), dma, dma,
            dma((2,)), dma((2, 8)),
            dma((2,)), dma((CH,)),
            dma, dma((CH, 3)),
            dma, dma((NS,)), dma((NS,)), dma((NS,)),
            dma((3,)), dma((3,)),
            dma((3,)), dma((3,)),
            dma, dma,
            dma((3,)), dma((3,)),
        ],
        compiler_params=pltpu.CompilerParams(collective_id=0, has_side_effects=True, vmem_limit_bytes=60 * 2**20),
        name="levels",
    )(mask_u, mask_l, parent, lu, ll, a, lp, du.reshape(16, deep, B), dl.reshape(16, deep, B))
    return place((x, d_u.reshape(B, B), y, y_p.reshape(B, B), d_l.reshape(B, B)))


def place_kernel(*refs):
    n = (len(refs) - 2) // 3
    sources, outs, held, sems_in, sems_out = refs[:n], refs[n:2 * n], refs[2 * n:3 * n], refs[-2], refs[-1]
    ins = [pltpu.make_async_copy(sources[i], held[i], sems_in.at[i]) for i in range(n)]
    puts = [pltpu.make_async_copy(held[i], outs[i], sems_out.at[i]) for i in range(n)]
    for copy in ins:
        copy.start()
    for i in range(n):
        ins[i].wait()
        puts[i].start()
    for copy in puts:
        copy.wait()


def place(arrays):
    n = len(arrays)
    hbm = pl.BlockSpec(memory_space=pltpu.HBM)
    return pl.pallas_call(
        place_kernel,
        out_shape=tuple(jax.ShapeDtypeStruct(v.shape, v.dtype) for v in arrays),
        in_specs=[hbm] * n,
        out_specs=(hbm,) * n,
        scratch_shapes=[pltpu.VMEM(v.shape, v.dtype) for v in arrays]
        + [pltpu.SemaphoreType.DMA((n,)), pltpu.SemaphoreType.DMA((n,))],
        compiler_params=pltpu.CompilerParams(vmem_limit_bytes=60 * 2**20),
        name="place",
    )(*arrays)


def solution(mesh):
    rows, cols = P(("grp", "row"), "col"), P(None, "col")
    none = P(None, None)
    return jax.shard_map(
        step,
        mesh=mesh,
        in_specs=(rows, rows, none, cols, rows, none, P(None), cols, cols),
        out_specs=(rows, cols, rows, cols, cols),
        check_vma=False,
    )
```

```python
import jax
import jax.numpy as jnp
from jax import lax
from jax.experimental import pallas as pl
from jax.experimental.pallas import tpu as pltpu
from jax.sharding import PartitionSpec as P

B = 256
H = 128
CH = 8
NS = 16
LAGS = (2, 4, 6)
UPPER = (13, 15, 18)
AHEAD = (2, 1)
MESH = pl.DeviceIdType.MESH
F32 = jnp.float32
BF16 = jnp.bfloat16


def device(g, x, h, b, z):
    return (g, z * 2 + h, b * 4 + x)


def swapped(n):
    return n % 2 == 1


def remote(src, dst, send, recv, target):
    return pltpu.make_async_remote_copy(
        src_ref=src, dst_ref=dst, send_sem=send, recv_sem=recv, device_id=target, device_id_type=MESH
    )


def took(ref, sem, target):
    remote(ref, ref, sem, sem, target).wait_recv()


def left_here(ref, sem, target):
    remote(ref, ref, sem, sem, target).wait_send()


def aligned(start, size):
    return pl.ds(pl.multiple_of(start, size), size)


def loop(lo, hi, f):
    def body(i, carry):
        f(i)
        return carry

    lax.fori_loop(lo, hi, body, 0)


def flipped(p, q):
    return lax.dot_general(p, q, (((0,), (0,)), ((), ())), preferred_element_type=F32)


def kernel(
    mask_u_in, mask_l_in, parent_in, lu_in, ll_in, a_in, lp_in, du_arg, dl_arg,
    x_out, y_out, du_out, yp_out, dl_out,
    mask_u, mask_l, parent, lu, ll, lp, du_in, dl_in, masked, a, s1, panel, part, r1, r2, kept, yb, xs, chosen_s, xst, ct, cl, red_s, red, dcol, back, y_held, du_held, yp_held, dl_held,
    in_sem, out_sem, as_sem, ar_sem, s1s, s1r, s2s, s2r, ags, agr, ps, p1r, p2r, p3r,
    ts, tr, rs, rr, cs, cr, gs, gr,
):
    g, row, col = lax.axis_index("grp"), lax.axis_index("row"), lax.axis_index("col")
    z, h, b, x = row // 2, row % 2, col // 4, col % 4
    me = g * 8 + row
    rows = a.shape[1]
    quarter, sl, half = rows // 4, rows // 8, rows // 2
    bl = min(B, rows)
    here = (g, row, col)

    arrivals_of = ((lu_in, lu), (ll_in, ll), (mask_u_in, mask_u), (mask_l_in, mask_l), (a_in, a.at[0]),
                   (parent_in, parent), (lp_in, lp), (du_arg, du_in), (dl_arg, dl_in))
    loads = [pltpu.make_async_copy(src, dst, in_sem.at[i]) for i, (src, dst) in enumerate(arrivals_of)]
    for load in loads:
        load.start()

    plane = [(0, dx, dy, 0) for dx in range(4) for dy in range(4)]
    line = [(dg, 0, dy, dz) for dg in range(2) for dy in (0, 2) for dz in range(4)]
    across = [(1, dx, db, 0) for dx in range(4) for db in (0, 5)]
    barrier = pltpu.get_barrier_semaphore()
    peers = []
    for dg, dx, dy, dz in plane + line + across:
        if dy == 5:
            key, ht, bt = (dg, dx, 5, dz), h, 1 - b
        else:
            y = (2 * h + b + dy) % 4
            key, ht, bt = (dg, dx, dy, dz), y // 2, y % 2
        if key != (0, 0, 0, 0) and key not in peers:
            peers.append(key)
            pl.semaphore_signal(
                barrier, inc=1, device_id=device((g + dg) % 2, (x + dx) % 4, ht, bt, (z + dz) % 4),
                device_id_type=MESH,
            )

    for load in loads[:4]:
        load.wait()
    for pn, (factor, mask) in enumerate(((lu, mask_u), (ll, mask_l))):
        for i in range(rows // bl):
            keep = mask[col, (me * rows + i * bl) // B] > 0
            values = factor[i * bl:(i + 1) * bl, :]
            masked[pn, i * bl:(i + 1) * bl, :] = jnp.where(keep, values, jnp.zeros_like(values))

    swap_a = remote(a.at[0], a.at[1], as_sem, ar_sem, (1 - g, row, col))
    pl.semaphore_wait(barrier, len(peers))

    def piece(pn, q, half_of):
        return masked.at[pn, aligned(q * quarter, quarter), aligned(half_of * H, H)]

    def first(pn, dz, dg):
        gt, zt = (g + dg) % 2, (z + dz) % 4
        return remote(
            piece(pn, zt, gt), s1.at[g, z, pn], s1s.at[pn], s1r.at[pn, g * 4 + z],
            device(gt, x, h, b, zt),
        )

    def first_in(pn, dz, dg):
        gf, zf = (g + dg) % 2, (z + dz) % 4
        return remote(piece(pn, z, g), s1.at[gf, zf, pn], s1s.at[pn], s1r.at[pn, gf * 4 + zf], here)

    order = [(dz, dg) for dz in (2, 1, 3, 0) for dg in (0, 1)]
    def hand_out(pn):
        for dz, dg in order:
            if (dz, dg) != (0, 0):
                first(pn, dz, dg).start()
        s1[g, z, pn] = masked[pn, aligned(z * quarter, quarter), aligned(g * H, H)]

    hand_out(0)
    hand_out(1)

    def spot_from(pn, hf, cf, lane):
        return (pn * 4 + cf // 2, aligned(hf * rows + z * quarter, quarter), lane)

    def second(pn, dz, dg, dh):
        zf, gf, ht = (z + dz) % 4, (g + dg) % 2, (h + dh) % 2
        stays = (zf == x) & (gf == b) & (ht == h)
        return stays, zf, gf, remote(
            s1.at[gf, zf, pn], panel.at[spot_from(pn, h, col, aligned((col % 2) * H, H))],
            s2s.at[pn], s2r.at[pn * 4 + col // 2], device(g, zf, ht, gf, z),
        )

    arrivals = [(dz, dg) for dz in (0, 1, 3, 2) for dg in (0, 1)]
    def pass_on(pn):
        for dz, dg in arrivals:
            if (dz, dg) != (0, 0):
                first_in(pn, dz, dg).wait_recv()
            for dh in range(2):
                stays, zf, gf, copy = second(pn, dz, dg, dh)
                pl.when(jnp.logical_not(stays))(copy.start)

                @pl.when(stays)
                def _(zf=zf, gf=gf):
                    panel[spot_from(pn, h, col, aligned((col % 2) * H, H))] = s1[gf, zf, pn]

    pass_on(0)
    loads[4].wait()
    swap_a.start()

    right, left = device(g, x, h, b, (z + 1) % 4), device(g, x, h, b, (z + 3) % 4)

    def gather(m, kind, q, hf, to):
        spot = panel.at[m, aligned(hf * rows + q * quarter, quarter)]
        return remote(spot, spot, ags, agr.at[m, kind], to)

    def step_a(m):
        own = col // 2 == m % 4
        pl.when(own)(lambda: took(panel.at[m, pl.ds(0, 3 * quarter // 2)], s2r.at[m], here))
        pl.when(jnp.logical_not(own))(lambda: took(panel.at[m, pl.ds(0, 2 * quarter)], s2r.at[m], here))
        gather(m, 0, z, 0, right).start()
        gather(m, 1, z, 1, left).start()
        gather(m, 2, z, 1, right).start()
        gather(m, 2, z, 0, left).start()

    def step_b(m):
        gather(m, 0, (z + 3) % 4, 0, right).wait_recv()
        gather(m, 2, (z + 3) % 4, 0, right).start()
        gather(m, 1, (z + 1) % 4, 1, left).wait_recv()
        gather(m, 2, (z + 1) % 4, 1, left).start()

    def step_w(m):
        took(panel.at[m, pl.ds(0, rows)], agr.at[m, 2], here)

    xr, xl = device(g, (x + 1) % 4, h, b, z), device(g, (x + 3) % 4, h, b, z)
    yp = device(g, x, h, 1 - b, z)
    far_x = (x + 2) % 4
    low = sl // 2

    def near(way):
        return (x + 1 + 2 * way) % 4

    def x_copy(src, dst, arrived, way):
        return remote(src, dst, ps, arrived, xl if way else xr)

    def half_even(n, way):
        return x_copy(part.at[n, way, far_x], r1.at[n, way], p1r.at[n], way)

    def half_odd(n, way):
        return x_copy(part.at[n, b, far_x, pl.ds(way * low, low)], r1.at[n, 0, pl.ds(way * low, low)], p1r.at[n], way)

    def full_even(n, way):
        return x_copy(part.at[n, :, near(way)], r2.at[n, way], p2r.at[n], way)

    def full_odd(n, way):
        return x_copy(part.at[n, b, near(way)], r2.at[n, 0, way], p2r.at[n], way)

    def pair_even(n):
        return remote(r2.at[n, 0, 1 - b], yb.at[n, 0], ps, p3r.at[n], yp)

    def pair_odd(n):
        return remote(part.at[n, 1 - b], yb.at[n], ps, p3r.at[n], yp)

    def add(p, q):
        return (p.astype(F32) + q.astype(F32)).astype(BF16)

    def by_parity(n, even, odd):
        pl.when(jnp.logical_not(swapped(n)))(lambda: even(n))
        pl.when(swapped(n))(lambda: odd(n))

    def step_c(n):
        m, o = n // 2, n % 2
        for bt in range(2):
            product = jnp.dot(
                a[o, bt * half:(bt + 1) * half, :], panel[m], preferred_element_type=F32
            ).astype(BF16)
            for xt in range(4):
                part[n, bt, xt] = product[xt * sl:(xt + 1) * sl]

        def even(n):
            half_even(n, 0).start()
            half_even(n, 1).start()

        by_parity(n, even, lambda n: pair_odd(n).start())

    def step_d(n):
        def even(n):
            took(r1.at[n], p1r.at[n], here)
            for way in range(2):
                part[n, way, near(way)] = add(part[n, way, near(way)], r1[n, way])
            full_even(n, 0).start()
            full_even(n, 1).start()

        def odd(n):
            pair_odd(n).wait_recv()
            for xt in range(4):
                part[n, b, xt] = add(part[n, b, xt], yb[n, xt])
            half_odd(n, 0).start()
            half_odd(n, 1).start()

        by_parity(n, even, odd)

    def step_e(n):
        def even(n):
            took(r2.at[n], p2r.at[n], here)
            for bt in range(2):
                total = part[n, bt, x].astype(F32) + r2[n, 0, bt].astype(F32) + r2[n, 1, bt].astype(F32)
                r2[n, 0, bt] = total.astype(BF16)

                @pl.when(b == bt)
                def _():
                    kept[n] = total

            pair_even(n).start()

        def odd(n):
            took(r1.at[n, 0], p1r.at[n], here)
            for way in range(2):
                spot = (n, b, near(way), pl.ds(way * low, low))
                part[spot] = add(part[spot], r1[n, 0, way * low:(way + 1) * low])
            full_odd(n, 0).start()
            full_odd(n, 1).start()

        by_parity(n, even, odd)

    def finish(n):
        def even(n):
            pair_even(n).wait_recv()
            kept[n] = -(kept[n] + yb[n, 0].astype(F32))

        def odd(n):
            took(r2.at[n, 0], p2r.at[n], here)
            kept[n] = -(part[n, b, x].astype(F32) + r2[n, 0, 0].astype(F32) + r2[n, 0, 1].astype(F32))

        by_parity(n, even, odd)
        return kept[n].astype(BF16)

    mine, lanes = aligned(col * sl, sl), aligned(g * H, H)

    def turn(pn, c, o):
        return remote(
            xs.at[pn * 8 + c, o], xst.at[pn, mine, lanes], ts.at[pn], tr.at[pn],
            ((g + o) % 2, row, c),
        )

    def wait_turned(dst, k):
        took(dst.at[pl.ds(0, 15 * sl // 2)], tr.at[k], here)

    def step_f(n):
        m, o = n // 2, n % 2
        pn = n // 8
        result = finish(n)
        for e in range(2):
            xs[2 * m + e, o] = result[:, e * H:(e + 1) * H]
        for e in range(2):
            c = 2 * (m % 4) + e
            self_turn = (c == col) & (o == 0)
            pl.when(jnp.logical_not(self_turn))(turn(pn, c, o).start)

            @pl.when(self_turn)
            def _():
                xst[pn, mine, lanes] = result[:, e * H:(e + 1) * H]

    def pick(i):
        c, o = (col + i // 2) % 8, i % 2
        return remote(
            chosen_s.at[c, o], ct.at[mine, lanes], ts.at[2], tr.at[2], ((g + o) % 2, row, c)
        )

    def peer(d):
        r = (me + d) % 16
        return r, (r // 8, r % 8, col)

    def scatter(k, d):
        r, to = peer(d)
        return remote(red_s.at[k, r], red.at[k, me], rs.at[k], rr.at[k], to)

    def reduce_start(k, value):
        red_s[k] = value.reshape(16, B // 16, B).astype(BF16)
        loop(1, 16, lambda d: scatter(k, d).start())
        red[k, me] = red_s[k, me]

    def reduce_end(k):
        took(red.at[k, pl.ds(0, 15)], rr.at[k], here)
        return jnp.sum(red[k].astype(F32), axis=0)

    outs = (du_held, yp_held, dl_held)
    x_put, y_put, du_put, yp_put, dl_put = [
        pltpu.make_async_copy(src, dst, out_sem.at[i])
        for i, (src, dst) in enumerate(
            ((xst.at[0], x_out), (y_held, y_out), (du_held, du_out), (yp_held, yp_out), (dl_held, dl_out))
        )
    ]

    def spread(k, d):
        r, to = peer(d)
        return remote(outs[k].at[me], outs[k].at[me], gs.at[k], gr.at[k], to)

    def spread_end(k):
        took(outs[k].at[pl.ds(0, 15)], gr.at[k], here)

    def column(d):
        return remote(dcol.at[col], dcol.at[col], cs, cr, (g, row, (col + d) % 8))

    def upper_1():
        for c in range(8):
            chosen_s[c] = xs[parent[c]]
        loop(1, 16, lambda i: pick(i).start())
        ct[mine, lanes] = chosen_s[col, 0]

    def upper_2():
        wait_turned(xst.at[0], 0)
        x_put.start()
        reduce_start(0, flipped(masked[0], xst[0]))
        wait_turned(ct, 2)
        reduce_start(1, flipped(ct[...], masked[1]))
        cl[...] = jnp.dot(ct[...], lp[...], preferred_element_type=F32)

    def upper_3():
        du = (du_in[me] - reduce_end(0)).astype(BF16)
        du_held[me] = du
        dcol[col] = du
        loop(1, 8, lambda d: column(d).start())
        loop(1, 16, lambda d: spread(0, d).start())

    def upper_4():
        crossed = reduce_end(1)
        took(dcol.at[pl.ds(0, 7)], cr, here)
        own = dcol[parent[col]]
        held = (-(crossed + jnp.dot(own, lp[...], preferred_element_type=F32))).astype(BF16)
        yp_held[me] = held
        loop(1, 16, lambda d: spread(1, d).start())
        back[...] = flipped(lp[aligned(me * (B // 16), B // 16), :], held)

    for load in loads[5:]:
        load.wait()
    step_a(0)
    step_a(1)
    step_b(0)
    pass_on(1)
    swap_a.wait_recv()

    def body(n, carry):
        m = n // 2
        starts = (n < NS) & (n % 2 == 0)

        def late():
            for lag, step in zip(LAGS, (step_d, step_e, step_f)):
                k = n - lag
                pl.when((k >= 0) & (k < NS))(lambda step=step, k=k: step(k))
            for at, step in zip(UPPER, (upper_1, upper_2, upper_3)):
                pl.when(n == at)(step)

        @pl.when(starts)
        def _():
            pl.when(m + AHEAD[0] < CH)(lambda: step_a(m + AHEAD[0]))
            pl.when(m + AHEAD[1] < CH)(lambda: step_b(m + AHEAD[1]))

        pl.when(starts)(lambda: step_w(m))
        pl.when(n < NS)(lambda: step_c(n))
        late()
        return carry

    lax.fori_loop(0, NS + LAGS[-1], body, 0)

    upper_4()
    wait_turned(xst.at[1], 1)
    y = (xst[1].astype(F32) - cl[...]).astype(BF16)
    y_held[...] = y
    y_put.start()
    reduce_start(2, flipped(masked[1], y) + back[...])
    dl_held[me] = (dl_in[me] - reduce_end(2)).astype(BF16)
    loop(1, 16, lambda d: spread(2, d).start())
    spread_end(0)
    du_put.start()
    spread_end(1)
    yp_put.start()

    swap_a.wait_send()
    for pn in range(2):
        left_here(panel.at[0, pl.ds(0, 7 * quarter // 2)], s1s.at[pn], here)
        left_here(panel.at[0, pl.ds(0, 15 * quarter // 2)], s2s.at[pn], here)
    left_here(panel.at[pl.ds(0, 6)], ags, here)
    left_here(panel.at[pl.ds(0, 7)], ps, here)
    for k in range(3):
        left_here(ct.at[pl.ds(0, 15 * sl // 2)], ts.at[k], here)
        left_here(red_s.at[k, pl.ds(0, 15)], rs.at[k], here)
        left_here(outs[k].at[pl.ds(0, 15)], gs.at[k], here)
    left_here(dcol.at[pl.ds(0, 7)], cs, here)
    spread_end(2)
    dl_put.start()
    for put in (x_put, y_put, du_put, yp_put, dl_put):
        put.wait()


def step(a, lu, mask_u, du, ll, mask_l, parent, lp, dl):
    rows, depth = a.shape
    quarter, sl, deep = rows // 4, rows // 8, B // 16
    dma = pltpu.SemaphoreType.DMA
    block = jax.ShapeDtypeStruct((rows, B), BF16)
    square = jax.ShapeDtypeStruct((16, deep, B), BF16)
    v = pltpu.VMEM
    x, y, d_u, y_p, d_l = pl.pallas_call(
        kernel,
        out_shape=(block, block, square, square, square),
        in_specs=[pl.BlockSpec(memory_space=pltpu.HBM)] * 9,
        out_specs=(pl.BlockSpec(memory_space=pltpu.HBM),) * 5,
        scratch_shapes=[
            pltpu.SMEM(mask_u.shape, jnp.int32),
            pltpu.SMEM(mask_l.shape, jnp.int32),
            pltpu.SMEM(parent.shape, jnp.int32),
            v((rows, B), BF16),
            v((rows, B), BF16),
            v((B, B), BF16),
            v((16, deep, B), F32),
            v((16, deep, B), F32),
            v((2, rows, B), BF16),
            v((2, rows, depth), BF16),
            v((2, 4, 2, quarter, H), BF16),
            v((CH, depth, B), BF16),
            v((NS, 2, 4, sl, B), BF16),
            v((NS, 2, sl, B), BF16),
            v((NS, 2, 2, sl, B), BF16),
            v((NS, sl, B), F32),
            v((NS, 4, sl, B), BF16),
            v((16, 2, sl, H), BF16),
            v((8, 2, sl, H), BF16),
            v((2, rows, B), BF16),
            v((rows, B), BF16),
            v((rows, B), F32),
            v((3, 16, deep, B), BF16),
            v((3, 16, deep, B), BF16),
            v((8, deep, B), BF16),
            v((B, B), F32),
            v((rows, B), BF16),
            v((16, deep, B), BF16),
            v((16, deep, B), BF16),
            v((16, deep, B), BF16),
            dma((9,)), dma((5,)), dma, dma,
            dma((2,)), dma((2, 8)),
            dma((2,)), dma((CH,)),
            dma, dma((CH, 3)),
            dma, dma((NS,)), dma((NS,)), dma((NS,)),
            dma((3,)), dma((3,)),
            dma((3,)), dma((3,)),
            dma, dma,
            dma((3,)), dma((3,)),
        ],
        compiler_params=pltpu.CompilerParams(collective_id=0, has_side_effects=True, vmem_limit_bytes=60 * 2**20),
        name="levels",
    )(mask_u, mask_l, parent, lu, ll, a, lp, du.reshape(16, deep, B), dl.reshape(16, deep, B))
    return place((x, d_u.reshape(B, B), y, y_p.reshape(B, B), d_l.reshape(B, B)))


def place_kernel(*refs):
    n = (len(refs) - 2) // 3
    sources, outs, held, sems_in, sems_out = refs[:n], refs[n:2 * n], refs[2 * n:3 * n], refs[-2], refs[-1]
    ins = [pltpu.make_async_copy(sources[i], held[i], sems_in.at[i]) for i in range(n)]
    puts = [pltpu.make_async_copy(held[i], outs[i], sems_out.at[i]) for i in range(n)]
    for copy in ins:
        copy.start()
    for i in range(n):
        ins[i].wait()
        puts[i].start()
    for copy in puts:
        copy.wait()


def place(arrays):
    n = len(arrays)
    hbm = pl.BlockSpec(memory_space=pltpu.HBM)
    return pl.pallas_call(
        place_kernel,
        out_shape=tuple(jax.ShapeDtypeStruct(v.shape, v.dtype) for v in arrays),
        in_specs=[hbm] * n,
        out_specs=(hbm,) * n,
        scratch_shapes=[pltpu.VMEM(v.shape, v.dtype) for v in arrays]
        + [pltpu.SemaphoreType.DMA((n,)), pltpu.SemaphoreType.DMA((n,))],
        compiler_params=pltpu.CompilerParams(vmem_limit_bytes=60 * 2**20),
        name="place",
    )(*arrays)


def solution(mesh):
    rows, cols = P(("grp", "row"), "col"), P(None, "col")
    none = P(None, None)
    return jax.shard_map(
        step,
        mesh=mesh,
        in_specs=(rows, rows, none, cols, rows, none, P(None), cols, cols),
        out_specs=(rows, cols, rows, cols, cols),
        check_vma=False,
    )
```

```python
import jax
import jax.numpy as jnp
from jax import lax
from jax.experimental import pallas as pl
from jax.experimental.pallas import tpu as pltpu
from jax.sharding import PartitionSpec as P

B = 256
H = 128
CH = 8
NS = 16
LAGS = (2, 4, 6)
UPPER = (13, 15, 18)
AHEAD = (2, 1)
MESH = pl.DeviceIdType.MESH
F32 = jnp.float32
BF16 = jnp.bfloat16


def device(g, x, h, b, z):
    return (g, z * 2 + h, b * 4 + x)


def swapped(n):
    return n % 2 == 1


def remote(src, dst, send, recv, target):
    return pltpu.make_async_remote_copy(
        src_ref=src, dst_ref=dst, send_sem=send, recv_sem=recv, device_id=target, device_id_type=MESH
    )


def took(ref, sem, target):
    remote(ref, ref, sem, sem, target).wait_recv()


def left_here(ref, sem, target):
    remote(ref, ref, sem, sem, target).wait_send()


def aligned(start, size):
    return pl.ds(pl.multiple_of(start, size), size)


def loop(lo, hi, f):
    def body(i, carry):
        f(i)
        return carry

    lax.fori_loop(lo, hi, body, 0)


def flipped(p, q):
    return lax.dot_general(p, q, (((0,), (0,)), ((), ())), preferred_element_type=F32)


def kernel(
    mask_u_in, mask_l_in, parent_in, lu_in, ll_in, a_in, lp_in, du_arg, dl_arg,
    x_out, y_out, du_out, yp_out, dl_out,
    mask_u, mask_l, parent, lu, ll, lp, du_in, dl_in, masked, a, s1, panel, part, r1, r2, kept, yb, xs, chosen_s, xst, ct, cl, red_s, red, dcol, back, y_held, du_held, yp_held, dl_held,
    in_sem, out_sem, as_sem, ar_sem, s1s, s1r, s2s, s2r, ags, agr, ps, p1r, p2r, p3r,
    ts, tr, rs, rr, cs, cr, gs, gr,
):
    g, row, col = lax.axis_index("grp"), lax.axis_index("row"), lax.axis_index("col")
    z, h, b, x = row // 2, row % 2, col // 4, col % 4
    me = g * 8 + row
    rows = a.shape[1]
    quarter, sl, half = rows // 4, rows // 8, rows // 2
    bl = min(B, rows)
    here = (g, row, col)

    arrivals_of = ((lu_in, lu), (ll_in, ll), (mask_u_in, mask_u), (mask_l_in, mask_l), (a_in, a.at[0]),
                   (parent_in, parent), (lp_in, lp), (du_arg, du_in), (dl_arg, dl_in))
    loads = [pltpu.make_async_copy(src, dst, in_sem.at[i]) for i, (src, dst) in enumerate(arrivals_of)]
    for load in loads:
        load.start()

    plane = [(0, dx, dy, 0) for dx in range(4) for dy in range(4)]
    line = [(dg, 0, dy, dz) for dg in range(2) for dy in (0, 2) for dz in range(4)]
    across = [(1, dx, db, 0) for dx in range(4) for db in (0, 5)]
    barrier = pltpu.get_barrier_semaphore()
    peers = []
    for dg, dx, dy, dz in plane + line + across:
        if dy == 5:
            key, ht, bt = (dg, dx, 5, dz), h, 1 - b
        else:
            y = (2 * h + b + dy) % 4
            key, ht, bt = (dg, dx, dy, dz), y // 2, y % 2
        if key != (0, 0, 0, 0) and key not in peers:
            peers.append(key)
            pl.semaphore_signal(
                barrier, inc=1, device_id=device((g + dg) % 2, (x + dx) % 4, ht, bt, (z + dz) % 4),
                device_id_type=MESH,
            )

    for load in loads[:4]:
        load.wait()
    for pn, (factor, mask) in enumerate(((lu, mask_u), (ll, mask_l))):
        for i in range(rows // bl):
            keep = mask[col, (me * rows + i * bl) // B] > 0
            values = factor[i * bl:(i + 1) * bl, :]
            masked[pn, i * bl:(i + 1) * bl, :] = jnp.where(keep, values, jnp.zeros_like(values))

    swap_a = remote(a.at[0], a.at[1], as_sem, ar_sem, (1 - g, row, col))
    pl.semaphore_wait(barrier, len(peers))

    def piece(pn, q, half_of):
        return masked.at[pn, aligned(q * quarter, quarter), aligned(half_of * H, H)]

    def first(pn, dz, dg):
        gt, zt = (g + dg) % 2, (z + dz) % 4
        return remote(
            piece(pn, zt, gt), s1.at[g, z, pn], s1s.at[pn], s1r.at[pn, g * 4 + z],
            device(gt, x, h, b, zt),
        )

    def first_in(pn, dz, dg):
        gf, zf = (g + dg) % 2, (z + dz) % 4
        return remote(piece(pn, z, g), s1.at[gf, zf, pn], s1s.at[pn], s1r.at[pn, gf * 4 + zf], here)

    order = [(dz, dg) for dz in (2, 1, 3, 0) for dg in (0, 1)]
    def hand_out(pn):
        for dz, dg in order:
            if (dz, dg) != (0, 0):
                first(pn, dz, dg).start()
        s1[g, z, pn] = masked[pn, aligned(z * quarter, quarter), aligned(g * H, H)]

    hand_out(0)
    hand_out(1)

    def spot_from(pn, hf, cf, lane):
        return (pn * 4 + cf // 2, aligned(hf * rows + z * quarter, quarter), lane)

    def second(pn, dz, dg, dh):
        zf, gf, ht = (z + dz) % 4, (g + dg) % 2, (h + dh) % 2
        stays = (zf == x) & (gf == b) & (ht == h)
        return stays, zf, gf, remote(
            s1.at[gf, zf, pn], panel.at[spot_from(pn, h, col, aligned((col % 2) * H, H))],
            s2s.at[pn], s2r.at[pn * 4 + col // 2], device(g, zf, ht, gf, z),
        )

    arrivals = [(dz, dg) for dz in (0, 1, 3, 2) for dg in (0, 1)]
    def pass_on(pn):
        for dz, dg in arrivals:
            if (dz, dg) != (0, 0):
                first_in(pn, dz, dg).wait_recv()
            for dh in range(2):
                stays, zf, gf, copy = second(pn, dz, dg, dh)
                pl.when(jnp.logical_not(stays))(copy.start)

                @pl.when(stays)
                def _(zf=zf, gf=gf):
                    panel[spot_from(pn, h, col, aligned((col % 2) * H, H))] = s1[gf, zf, pn]

    pass_on(0)
    loads[4].wait()
    swap_a.start()

    right, left = device(g, x, h, b, (z + 1) % 4), device(g, x, h, b, (z + 3) % 4)

    def gather(m, kind, q, hf, to):
        spot = panel.at[m, aligned(hf * rows + q * quarter, quarter)]
        return remote(spot, spot, ags, agr.at[m, kind], to)

    def step_a(m):
        own = col // 2 == m % 4
        pl.when(own)(lambda: took(panel.at[m, pl.ds(0, 3 * quarter // 2)], s2r.at[m], here))
        pl.when(jnp.logical_not(own))(lambda: took(panel.at[m, pl.ds(0, 2 * quarter)], s2r.at[m], here))
        gather(m, 0, z, 0, right).start()
        gather(m, 1, z, 1, left).start()
        gather(m, 2, z, 1, right).start()
        gather(m, 2, z, 0, left).start()

    def step_b(m):
        gather(m, 0, (z + 3) % 4, 0, right).wait_recv()
        gather(m, 2, (z + 3) % 4, 0, right).start()
        gather(m, 1, (z + 1) % 4, 1, left).wait_recv()
        gather(m, 2, (z + 1) % 4, 1, left).start()

    def step_w(m):
        took(panel.at[m, pl.ds(0, rows)], agr.at[m, 2], here)

    xr, xl = device(g, (x + 1) % 4, h, b, z), device(g, (x + 3) % 4, h, b, z)
    yp = device(g, x, h, 1 - b, z)
    far_x = (x + 2) % 4
    low = sl // 2

    def near(way):
        return (x + 1 + 2 * way) % 4

    def x_copy(src, dst, arrived, way):
        return remote(src, dst, ps, arrived, xl if way else xr)

    def half_even(n, way):
        return x_copy(part.at[n, way, far_x], r1.at[n, way], p1r.at[n], way)

    def half_odd(n, way):
        return x_copy(part.at[n, b, far_x, pl.ds(way * low, low)], r1.at[n, 0, pl.ds(way * low, low)], p1r.at[n], way)

    def full_even(n, way):
        return x_copy(part.at[n, :, near(way)], r2.at[n, way], p2r.at[n], way)

    def full_odd(n, way):
        return x_copy(part.at[n, b, near(way)], r2.at[n, 0, way], p2r.at[n], way)

    def pair_even(n):
        return remote(r2.at[n, 0, 1 - b], yb.at[n, 0], ps, p3r.at[n], yp)

    def pair_odd(n):
        return remote(part.at[n, 1 - b], yb.at[n], ps, p3r.at[n], yp)

    def add(p, q):
        return (p.astype(F32) + q.astype(F32)).astype(BF16)

    def by_parity(n, even, odd):
        pl.when(jnp.logical_not(swapped(n)))(lambda: even(n))
        pl.when(swapped(n))(lambda: odd(n))

    def step_c(n):
        m, o = n // 2, n % 2
        for bt in range(2):
            product = jnp.dot(
                a[o, bt * half:(bt + 1) * half, :], panel[m], preferred_element_type=F32
            ).astype(BF16)
            for xt in range(4):
                part[n, bt, xt] = product[xt * sl:(xt + 1) * sl]

        def even(n):
            half_even(n, 0).start()
            half_even(n, 1).start()

        by_parity(n, even, lambda n: pair_odd(n).start())

    def step_d(n):
        def even(n):
            took(r1.at[n], p1r.at[n], here)
            for way in range(2):
                part[n, way, near(way)] = add(part[n, way, near(way)], r1[n, way])
            full_even(n, 0).start()
            full_even(n, 1).start()

        def odd(n):
            pair_odd(n).wait_recv()
            for xt in range(4):
                part[n, b, xt] = add(part[n, b, xt], yb[n, xt])
            half_odd(n, 0).start()
            half_odd(n, 1).start()

        by_parity(n, even, odd)

    def step_e(n):
        def even(n):
            took(r2.at[n], p2r.at[n], here)
            for bt in range(2):
                total = part[n, bt, x].astype(F32) + r2[n, 0, bt].astype(F32) + r2[n, 1, bt].astype(F32)
                r2[n, 0, bt] = total.astype(BF16)

                @pl.when(b == bt)
                def _():
                    kept[n] = total

            pair_even(n).start()

        def odd(n):
            took(r1.at[n, 0], p1r.at[n], here)
            for way in range(2):
                spot = (n, b, near(way), pl.ds(way * low, low))
                part[spot] = add(part[spot], r1[n, 0, way * low:(way + 1) * low])
            full_odd(n, 0).start()
            full_odd(n, 1).start()

        by_parity(n, even, odd)

    def finish(n):
        def even(n):
            pair_even(n).wait_recv()
            kept[n] = -(kept[n] + yb[n, 0].astype(F32))

        def odd(n):
            took(r2.at[n, 0], p2r.at[n], here)
            kept[n] = -(part[n, b, x].astype(F32) + r2[n, 0, 0].astype(F32) + r2[n, 0, 1].astype(F32))

        by_parity(n, even, odd)
        return kept[n].astype(BF16)

    mine, lanes = aligned(col * sl, sl), aligned(g * H, H)

    def turn(pn, c, o):
        return remote(
            xs.at[pn * 8 + c, o], xst.at[pn, mine, lanes], ts.at[pn], tr.at[pn],
            ((g + o) % 2, row, c),
        )

    def wait_turned(dst, k):
        took(dst.at[pl.ds(0, 15 * sl // 2)], tr.at[k], here)

    def step_f(n):
        m, o = n // 2, n % 2
        pn = n // 8
        result = finish(n)
        for e in range(2):
            xs[2 * m + e, o] = result[:, e * H:(e + 1) * H]
        for e in range(2):
            c = 2 * (m % 4) + e
            self_turn = (c == col) & (o == 0)
            pl.when(jnp.logical_not(self_turn))(turn(pn, c, o).start)

            @pl.when(self_turn)
            def _():
                xst[pn, mine, lanes] = result[:, e * H:(e + 1) * H]

    def pick(i):
        c, o = (col + i // 2) % 8, i % 2
        return remote(
            chosen_s.at[c, o], ct.at[mine, lanes], ts.at[2], tr.at[2], ((g + o) % 2, row, c)
        )

    def peer(d):
        r = (me + 5 * d) % 16
        return r, (r // 8, r % 8, col)

    def scatter(k, d):
        r, to = peer(d)
        return remote(red_s.at[k, r], red.at[k, me], rs.at[k], rr.at[k], to)

    def reduce_start(k, value):
        red_s[k] = value.reshape(16, B // 16, B).astype(BF16)
        loop(1, 16, lambda d: scatter(k, d).start())
        red[k, me] = red_s[k, me]

    def reduce_end(k):
        took(red.at[k, pl.ds(0, 15)], rr.at[k], here)
        return jnp.sum(red[k].astype(F32), axis=0)

    outs = (du_held, yp_held, dl_held)
    x_put, y_put, du_put, yp_put, dl_put = [
        pltpu.make_async_copy(src, dst, out_sem.at[i])
        for i, (src, dst) in enumerate(
            ((xst.at[0], x_out), (y_held, y_out), (du_held, du_out), (yp_held, yp_out), (dl_held, dl_out))
        )
    ]

    def spread(k, d):
        r, to = peer(d)
        return remote(outs[k].at[me], outs[k].at[me], gs.at[k], gr.at[k], to)

    def spread_end(k):
        took(outs[k].at[pl.ds(0, 15)], gr.at[k], here)

    def column(d):
        return remote(dcol.at[col], dcol.at[col], cs, cr, (g, row, (col + d) % 8))

    def upper_1():
        for c in range(8):
            chosen_s[c] = xs[parent[c]]
        loop(1, 16, lambda i: pick(i).start())
        ct[mine, lanes] = chosen_s[col, 0]

    def upper_2():
        wait_turned(xst.at[0], 0)
        x_put.start()
        reduce_start(0, flipped(masked[0], xst[0]))
        wait_turned(ct, 2)
        reduce_start(1, flipped(ct[...], masked[1]))
        cl[...] = jnp.dot(ct[...], lp[...], preferred_element_type=F32)

    def upper_3():
        du = (du_in[me] - reduce_end(0)).astype(BF16)
        du_held[me] = du
        dcol[col] = du
        loop(1, 8, lambda d: column(d).start())
        loop(1, 16, lambda d: spread(0, d).start())

    def upper_4():
        crossed = reduce_end(1)
        took(dcol.at[pl.ds(0, 7)], cr, here)
        own = dcol[parent[col]]
        held = (-(crossed + jnp.dot(own, lp[...], preferred_element_type=F32))).astype(BF16)
        yp_held[me] = held
        loop(1, 16, lambda d: spread(1, d).start())
        back[...] = flipped(lp[aligned(me * (B // 16), B // 16), :], held)

    for load in loads[5:]:
        load.wait()
    step_a(0)
    step_a(1)
    step_b(0)
    pass_on(1)
    swap_a.wait_recv()

    def body(n, carry):
        m = n // 2
        starts = (n < NS) & (n % 2 == 0)

        def late():
            for lag, step in zip(LAGS, (step_d, step_e, step_f)):
                k = n - lag
                pl.when((k >= 0) & (k < NS))(lambda step=step, k=k: step(k))
            for at, step in zip(UPPER, (upper_1, upper_2, upper_3)):
                pl.when(n == at)(step)

        @pl.when(starts)
        def _():
            pl.when(m + AHEAD[0] < CH)(lambda: step_a(m + AHEAD[0]))
            pl.when(m + AHEAD[1] < CH)(lambda: step_b(m + AHEAD[1]))

        pl.when(starts)(lambda: step_w(m))
        pl.when(n < NS)(lambda: step_c(n))
        late()
        return carry

    lax.fori_loop(0, NS + LAGS[-1], body, 0)

    upper_4()
    wait_turned(xst.at[1], 1)
    y = (xst[1].astype(F32) - cl[...]).astype(BF16)
    y_held[...] = y
    y_put.start()
    reduce_start(2, flipped(masked[1], y) + back[...])
    dl_held[me] = (dl_in[me] - reduce_end(2)).astype(BF16)
    loop(1, 16, lambda d: spread(2, d).start())
    spread_end(0)
    du_put.start()
    spread_end(1)
    yp_put.start()

    swap_a.wait_send()
    for pn in range(2):
        left_here(panel.at[0, pl.ds(0, 7 * quarter // 2)], s1s.at[pn], here)
        left_here(panel.at[0, pl.ds(0, 15 * quarter // 2)], s2s.at[pn], here)
    left_here(panel.at[pl.ds(0, 6)], ags, here)
    left_here(panel.at[pl.ds(0, 7)], ps, here)
    for k in range(3):
        left_here(ct.at[pl.ds(0, 15 * sl // 2)], ts.at[k], here)
        left_here(red_s.at[k, pl.ds(0, 15)], rs.at[k], here)
        left_here(outs[k].at[pl.ds(0, 15)], gs.at[k], here)
    left_here(dcol.at[pl.ds(0, 7)], cs, here)
    spread_end(2)
    dl_put.start()
    for put in (x_put, y_put, du_put, yp_put, dl_put):
        put.wait()


def step(a, lu, mask_u, du, ll, mask_l, parent, lp, dl):
    rows, depth = a.shape
    quarter, sl, deep = rows // 4, rows // 8, B // 16
    dma = pltpu.SemaphoreType.DMA
    block = jax.ShapeDtypeStruct((rows, B), BF16)
    square = jax.ShapeDtypeStruct((16, deep, B), BF16)
    v = pltpu.VMEM
    x, y, d_u, y_p, d_l = pl.pallas_call(
        kernel,
        out_shape=(block, block, square, square, square),
        in_specs=[pl.BlockSpec(memory_space=pltpu.HBM)] * 9,
        out_specs=(pl.BlockSpec(memory_space=pltpu.HBM),) * 5,
        scratch_shapes=[
            pltpu.SMEM(mask_u.shape, jnp.int32),
            pltpu.SMEM(mask_l.shape, jnp.int32),
            pltpu.SMEM(parent.shape, jnp.int32),
            v((rows, B), BF16),
            v((rows, B), BF16),
            v((B, B), BF16),
            v((16, deep, B), F32),
            v((16, deep, B), F32),
            v((2, rows, B), BF16),
            v((2, rows, depth), BF16),
            v((2, 4, 2, quarter, H), BF16),
            v((CH, depth, B), BF16),
            v((NS, 2, 4, sl, B), BF16),
            v((NS, 2, sl, B), BF16),
            v((NS, 2, 2, sl, B), BF16),
            v((NS, sl, B), F32),
            v((NS, 4, sl, B), BF16),
            v((16, 2, sl, H), BF16),
            v((8, 2, sl, H), BF16),
            v((2, rows, B), BF16),
            v((rows, B), BF16),
            v((rows, B), F32),
            v((3, 16, deep, B), BF16),
            v((3, 16, deep, B), BF16),
            v((8, deep, B), BF16),
            v((B, B), F32),
            v((rows, B), BF16),
            v((16, deep, B), BF16),
            v((16, deep, B), BF16),
            v((16, deep, B), BF16),
            dma((9,)), dma((5,)), dma, dma,
            dma((2,)), dma((2, 8)),
            dma((2,)), dma((CH,)),
            dma, dma((CH, 3)),
            dma, dma((NS,)), dma((NS,)), dma((NS,)),
            dma((3,)), dma((3,)),
            dma((3,)), dma((3,)),
            dma, dma,
            dma((3,)), dma((3,)),
        ],
        compiler_params=pltpu.CompilerParams(collective_id=0, has_side_effects=True, vmem_limit_bytes=60 * 2**20),
        name="levels",
    )(mask_u, mask_l, parent, lu, ll, a, lp, du.reshape(16, deep, B), dl.reshape(16, deep, B))
    return place((x, d_u.reshape(B, B), y, y_p.reshape(B, B), d_l.reshape(B, B)))


def place_kernel(*refs):
    n = (len(refs) - 2) // 3
    sources, outs, held, sems_in, sems_out = refs[:n], refs[n:2 * n], refs[2 * n:3 * n], refs[-2], refs[-1]
    ins = [pltpu.make_async_copy(sources[i], held[i], sems_in.at[i]) for i in range(n)]
    puts = [pltpu.make_async_copy(held[i], outs[i], sems_out.at[i]) for i in range(n)]
    for copy in ins:
        copy.start()
    for i in range(n):
        ins[i].wait()
        puts[i].start()
    for copy in puts:
        copy.wait()


def place(arrays):
    n = len(arrays)
    hbm = pl.BlockSpec(memory_space=pltpu.HBM)
    return pl.pallas_call(
        place_kernel,
        out_shape=tuple(jax.ShapeDtypeStruct(v.shape, v.dtype) for v in arrays),
        in_specs=[hbm] * n,
        out_specs=(hbm,) * n,
        scratch_shapes=[pltpu.VMEM(v.shape, v.dtype) for v in arrays]
        + [pltpu.SemaphoreType.DMA((n,)), pltpu.SemaphoreType.DMA((n,))],
        compiler_params=pltpu.CompilerParams(vmem_limit_bytes=60 * 2**20),
        name="place",
    )(*arrays)


def solution(mesh):
    rows, cols = P(("grp", "row"), "col"), P(None, "col")
    none = P(None, None)
    return jax.shard_map(
        step,
        mesh=mesh,
        in_specs=(rows, rows, none, cols, rows, none, P(None), cols, cols),
        out_specs=(rows, cols, rows, cols, cols),
        check_vma=False,
    )
```
